16 devices in a mesh: dp: 16 (over z, y, x, core).
Axes of the slice: x: 2, y: 2, z: 2, core: 2. Of those that a mesh axis runs over, the one named last changes fastest.
Arguments:
- hidden: bfloat16 [32768, 6144], P('dp')
- router_w: bfloat16 [6144, 160], replicated
- expert_idx: int32 [32768, 8], P('dp')
- gate_grad: float32 [32768, 8], P('dp')
Outputs:
- output 1: float32 [32768, 8], P('dp')
- output 2: float32 [], replicated
- output 3: bfloat16 [32768, 6144], P('dp')
- output 4: float32 [6144, 160], replicated
All inputs are finite; a program needn't handle non-finite values.
Results may differ from the reference program's by a relative error of at most 0.0078759.
Values sent between devices are 32-bit elements.
A program may use at most 1 GiB of HBM per device.

```python
import jax
import jax.numpy as jnp
from jax import lax

TOKENS = 32768
HIDDEN = 6144
EXPERTS = 160
TOP_K = 8
SHARDS = 16
ALPHA = 0.001
ROWS_PER_SHARD = TOKENS // SHARDS
LOSS_SCALE = float(TOKENS * EXPERTS * EXPERTS)


def draw_routes(key):
    key_bias, key_noise, key_shift = jax.random.split(key, 3)
    shard_bias = jax.random.randint(key_bias, (SHARDS, EXPERTS), 0, 48)
    row_noise = jax.random.randint(key_noise, (TOKENS, EXPERTS), 0, 32)
    row_shift = jax.random.randint(key_shift, (SHARDS, 1), 0, EXPERTS)
    row_pos = jnp.arange(ROWS_PER_SHARD)[None, :] + row_shift
    forced = (row_pos % EXPERTS).reshape(TOKENS, 1)
    expert_ids = jnp.arange(EXPERTS)[None, :]
    scores = jnp.repeat(shard_bias, ROWS_PER_SHARD, axis=0) + row_noise + 1000 * (expert_ids == forced).astype(jnp.int32)
    scores = scores * EXPERTS + expert_ids
    chosen = lax.top_k(scores, TOP_K)[1]
    return chosen.astype(jnp.int32)


def setup_inputs(seed: int = 0) -> dict:
    keys = jax.random.split(jax.random.key(seed), 5)
    shard_mean = 0.5 * jax.random.normal(keys[0], (SHARDS, HIDDEN), jnp.float32)
    hidden = jax.random.normal(keys[1], (TOKENS, HIDDEN), jnp.float32) + jnp.repeat(shard_mean, ROWS_PER_SHARD, axis=0)
    router_w = jax.random.normal(keys[2], (HIDDEN, EXPERTS), jnp.float32) * HIDDEN ** -0.5
    expert_idx = draw_routes(keys[3])
    grad_scale = ALPHA * TOP_K * TOP_K / (TOKENS * EXPERTS)
    gate_grad = jax.random.normal(keys[4], (TOKENS, TOP_K), jnp.float32) * grad_scale
    return {"hidden": hidden.astype(jnp.bfloat16), "router_w": router_w.astype(jnp.bfloat16), "expert_idx": expert_idx, "gate_grad": gate_grad}


def reference(hidden, router_w, expert_idx, gate_grad):
    logits = jnp.dot(hidden, router_w, preferred_element_type=jnp.float32)
    expert_freq = jnp.bincount(expert_idx.reshape(-1), length=EXPERTS).astype(jnp.float32) / TOKENS

    def objective(logit_vals):
        router_probs = jax.nn.softmax(logit_vals, axis=-1)
        picked = jnp.take_along_axis(router_probs, expert_idx, axis=1)
        gate_probs = picked / jnp.sum(picked, axis=1, keepdims=True)
        aux_loss = ALPHA * EXPERTS * jnp.sum(expert_freq * jnp.mean(router_probs, axis=0))
        return gate_probs, aux_loss

    (gate_probs, aux_loss), pullback = jax.vjp(objective, logits)
    logit_grad = pullback((LOSS_SCALE * gate_grad, jnp.asarray(LOSS_SCALE, jnp.float32)))[0]
    grad_bf = logit_grad.astype(jnp.bfloat16)
    hidden_grad = jnp.dot(grad_bf, router_w.T, preferred_element_type=jnp.float32).astype(jnp.bfloat16)
    router_grad = jnp.dot(hidden.T, grad_bf, preferred_element_type=jnp.float32)
    return gate_probs, aux_loss, hidden_grad, router_grad
```

```python
import functools

import jax
import jax.numpy as jnp
from jax import lax
from jax.experimental import pallas as pl
from jax.experimental.pallas import tpu as pltpu
from jax.sharding import PartitionSpec as P

LOSS_ALPHA = 0.001
MESH = pl.DeviceIdType.MESH
TB = 512
SLAB = 256
LAG = 2
ANY = pl.BlockSpec(memory_space=pl.ANY)
VMEM = pl.BlockSpec(memory_space=pltpu.VMEM)


def first_kernel(total_rows, num_devices, hid_hbm, wt_hbm, idx_ref, gg_ref,
                 gt_ref, gates_ref, aux_ref, out_ref,
                 hid, wt, probs, pgrad, psum, flane, cnts, auxs, part, dbuf, rx,
                 hsem, wsem, csend, crecv, asend, arecv, dsend, drecv, xsend, xrecv, gsend, grecv, esend, erecv):
    tokens, width = hid.shape
    experts = wt.shape[0]
    half = experts // 2
    nblk = tokens // TB
    loss_scale = float(total_rows * experts * experts)
    aux_coef = loss_scale * LOSS_ALPHA * experts / total_rows

    me = lax.axis_index("dp")
    core, bx, by, bz = me % 2, (me // 2) % 2, (me // 4) % 2, me // 8
    partner = me + 1 - 2 * core
    across = {"x": me + 2 - 4 * bx, "y": me + 4 - 8 * by, "z": me + 8 - 16 * bz}
    bits = {"x": bx, "y": by, "z": bz}
    routes = (("x", "y", "z"), ("y", "z", "x"), ("z", "x", "y"))
    mine = pl.ds(pl.multiple_of(core * half, 8), half)
    theirs = pl.ds(pl.multiple_of((1 - core) * half, 8), half)

    def hid_copy(b):
        rows = pl.ds(pl.multiple_of(b * TB, TB), TB)
        return pltpu.make_async_copy(hid_hbm.at[rows], hid.at[rows], hsem.at[b])

    w_copy = pltpu.make_async_copy(wt_hbm, wt, wsem)
    w_copy.start()
    for b in range(nblk):
        hid_copy(b).start()

    barrier = pltpu.get_barrier_semaphore()
    for d in range(1, num_devices):
        pl.semaphore_signal(barrier, inc=1, device_id=((me + d) % num_devices,), device_id_type=MESH)

    erows = cnts.shape[2]
    eids = lax.broadcasted_iota(jnp.int32, (erows, 128), 0)

    def count(i, acc):
        ids = idx_ref[:, pl.ds(pl.multiple_of(i * 128, 128), 128)]
        for j in range(ids.shape[0]):
            acc = acc + jnp.where(eids == ids[j:j + 1, :], 1.0, 0.0)
        return acc

    local = lax.fori_loop(0, tokens // 128, count, jnp.zeros((erows, 128), jnp.float32))
    row = jnp.sum(local.T, axis=0, keepdims=True)
    cnts[0] = jnp.broadcast_to(row, (8, erows))
    pl.semaphore_wait(barrier, num_devices - 1)

    def spread(buf, send, recv):
        copies = []
        for d in range(1, num_devices):
            copies.append(pltpu.make_async_remote_copy(
                buf.at[0], buf.at[d], send.at[d], recv.at[d],
                device_id=((me + d) % num_devices,), device_id_type=MESH))
        for c in copies:
            c.start()
        return copies

    count_copies = spread(cnts, csend, crecv)
    psum[...] = jnp.zeros_like(psum)
    w_copy.wait()

    def cols(b):
        return pl.ds(pl.multiple_of(b * TB, TB), TB)

    def logits(b):
        hid_copy(b).wait()
        rows = cols(b)
        probs[:, rows] = lax.dot_general(wt[...], hid[rows, :], (((1,), (1,)), ((), ())),
                                         preferred_element_type=jnp.float32)

    ids_e = lax.broadcasted_iota(jnp.int32, (experts, TB), 0)

    def forward(b):
        c = cols(b)
        lg = probs[:, c]
        ex = jnp.exp(lg - jnp.max(lg, axis=0, keepdims=True))
        p = ex / jnp.sum(ex, axis=0, keepdims=True)
        probs[:, c] = p
        ids = idx_ref[:, c]
        picked = jnp.concatenate(
            [jnp.sum(jnp.where(ids_e == ids[j:j + 1, :], p, 0.0), axis=0, keepdims=True)
             for j in range(ids.shape[0])], axis=0)
        pick_sum = jnp.sum(picked, axis=0, keepdims=True)
        gates = picked / pick_sum
        gates_ref[:, c] = gates
        sg = loss_scale * gg_ref[:, c]
        pgrad[:, c] = (sg - jnp.sum(sg * gates, axis=0, keepdims=True)) / pick_sum
        acc = p[:, 0:128]
        for i in range(1, TB // 128):
            acc = acc + p[:, i * 128:(i + 1) * 128]
        psum[...] += acc

    def backward(b):
        c = cols(b)
        p = probs[:, c]
        ids = idx_ref[:, c]
        pg = pgrad[:, c]
        f = flane[...]
        prob_grad = jnp.zeros_like(p)
        for j in range(ids.shape[0]):
            prob_grad = jnp.where(ids_e == ids[j:j + 1, :], pg[j:j + 1, :], prob_grad)
        prob_grad = prob_grad + aux_coef * jnp.concatenate([f] * (TB // 128), axis=1)
        inner = jnp.sum(p * prob_grad, axis=0, keepdims=True)
        gt_ref[:, c] = (p * (prob_grad - inner)).astype(jnp.bfloat16)

    logits(0)
    for b in range(1, nblk):
        logits(b)
        forward(b - 1)
        if b == nblk - 2:
            for cp in count_copies:
                cp.wait()
            tot = cnts[0]
            for d in range(1, num_devices):
                tot = tot + cnts[d]
            freq = tot[0:1, :] / total_rows
            flane[...] = jnp.broadcast_to(freq, (128, erows)).T[:experts, :]
            for bb in range(b):
                backward(bb)
        elif b > nblk - 2:
            backward(b - 1)
    forward(nblk - 1)
    backward(nblk - 1)

    def slab(p, k):
        flips = ((7 - k) // 4, ((7 - k) // 2) % 2, (7 - k) % 2)
        v = {}
        for name, fl in zip(routes[p], flips):
            v[name] = 1 - bits[name] if fl else bits[name]
        return p * 8 + v["z"] * 4 + v["y"] * 2 + v["x"]

    def dcopy(p, k):
        s = slab(p, k)
        return pltpu.make_async_remote_copy(part.at[s, theirs], dbuf.at[p * 8 + k], dsend.at[p * 8 + k],
                                            drecv.at[p * 8 + k], device_id=(partner,), device_id_type=MESH)

    def xcopy(p, k):
        to = across[routes[p][0 if k < 4 else 1 if k < 6 else 2]]
        return pltpu.make_async_remote_copy(part.at[slab(p, k), mine], rx.at[p * 7 + k], xsend.at[p * 7 + k],
                                            xrecv.at[p * 7 + k], device_id=(to,), device_id_type=MESH)

    def gcopy(p, k, dim):
        s = slab(p, k)
        j = k - (4, 2, 1)[dim]
        return pltpu.make_async_remote_copy(out_ref.at[s, mine], out_ref.at[s, mine], gsend.at[p * 7 + j],
                                            grecv.at[p * 7 + j], device_id=(across[routes[p][dim]],),
                                            device_id_type=MESH)

    def ecopy(p, k):
        s = slab(p, k)
        return pltpu.make_async_remote_copy(out_ref.at[s, mine], out_ref.at[s, mine], esend.at[p * 8 + k],
                                            erecv.at[p * 8 + k], device_id=(partner,), device_id_type=MESH)

    def compute(p, k):
        s = slab(p, k)
        part[s] = jnp.dot(gt_ref[...], hid[:, pl.ds(pl.multiple_of(s * SLAB, SLAB), SLAB)],
                          preferred_element_type=jnp.float32)
        dcopy(p, k).start()

    def reduce_first(k):
        for p in range(3):
            s = slab(p, k)
            dcopy(p, k).wait_recv()
            part[s, mine] = part[s, mine] + dbuf[p * 8 + k]
            if k < 4:
                xcopy(p, k).start()

    for k in range(8):
        for p in range(3):
            compute(p, k)
        if k >= LAG:
            reduce_first(k - LAG)
        if k == 2:
            auxs[0] = jnp.broadcast_to(jnp.sum(psum[...] * flane[...]), (8, 128))
            aux_copies = spread(auxs, asend, arecv)
    for k in range(8 - LAG, 8):
        reduce_first(k)

    for k in (4, 5, 6):
        for p in range(3):
            s = slab(p, k)
            xcopy(p, k - 4).wait_recv()
            acc = part[s, mine] + rx[p * 7 + k - 4]
            if k == 6:
                xcopy(p, 4).wait_recv()
                acc = acc + rx[p * 7 + 4]
            part[s, mine] = acc
            xcopy(p, k).start()
    for p in range(3):
        s = slab(p, 7)
        for i in (3, 5, 6):
            xcopy(p, i).wait_recv()
        out_ref[s, mine] = part[s, mine] + rx[p * 7 + 3] + rx[p * 7 + 5] + rx[p * 7 + 6]
        for dim in (2, 1, 0):
            gcopy(p, 7, dim).start()
        ecopy(p, 7).start()
    for k in (6, 5, 4, 3, 2, 1, 0):
        for p in range(3):
            gcopy(p, k + (1 if k == 6 else 2 if k >= 4 else 4), 2 if k == 6 else 1 if k >= 4 else 0).wait_recv()
            if k == 6:
                gcopy(p, 6, 1).start()
            if k >= 4:
                gcopy(p, k, 0).start()
            ecopy(p, k).start()

    for cp in aux_copies:
        cp.wait()
    tot = auxs[0]
    for d in range(1, num_devices):
        tot = tot + auxs[d]
    aux_ref[...] = tot * (LOSS_ALPHA * experts / total_rows)

    for k in range(8):
        for p in range(3):
            dcopy(p, k).wait_send()
            if k < 7:
                xcopy(p, k).wait_send()
            ecopy(p, k).wait()
    for p in range(3):
        for k, dims in ((7, (0, 1, 2)), (6, (0, 1)), (5, (0,)), (4, (0,))):
            for dim in dims:
                gcopy(p, k, dim).wait_send()


def second_kernel(gt_ref, wt_ref, gates_in, aux_in, rg_in, hg_ref, gates_out, aux_out, rg_out, g_scr, sems):
    i = pl.program_id(0)
    rows = hg_ref.shape[0]
    slabs = rg_in.shape[0]
    others = [pltpu.make_async_copy(gates_in, gates_out, sems.at[slabs]),
              pltpu.make_async_copy(aux_in.at[pl.ds(0, 1)], aux_out, sems.at[slabs + 1])]
    others += [pltpu.make_async_copy(rg_in.at[s], rg_out.at[:, pl.ds(s * SLAB, SLAB)], sems.at[s])
               for s in range(slabs)]

    @pl.when(i == 0)
    def _():
        for c in others:
            c.start()

    g = gt_ref[:, pl.ds(pl.multiple_of(i * rows, rows), rows)].T
    hg_ref[...] = jnp.dot(g, wt_ref[...], preferred_element_type=jnp.float32).astype(jnp.bfloat16)

    @pl.when(i == pl.num_programs(0) - 1)
    def _():
        for c in others:
            c.wait()


def solution(mesh):
    n = mesh.shape["dp"]

    def device_step(hidden, router_w, expert_idx, gate_grad):
        tokens, width = hidden.shape
        experts = router_w.shape[1]
        top_k = expert_idx.shape[1]
        slabs = width // SLAB
        half = experts // 2
        f32 = jnp.float32
        wt = router_w.T
        gt, gates, aux, rg = pl.pallas_call(
            functools.partial(first_kernel, tokens * n, n),
            out_shape=(jax.ShapeDtypeStruct((experts, tokens), jnp.bfloat16),
                       jax.ShapeDtypeStruct((top_k, tokens), f32),
                       jax.ShapeDtypeStruct((8, 128), f32),
                       jax.ShapeDtypeStruct((slabs, experts, SLAB), f32)),
            in_specs=[ANY, ANY, VMEM, VMEM],
            out_specs=(VMEM, VMEM, VMEM, VMEM),
            scratch_shapes=[
                pltpu.VMEM((tokens, width), jnp.bfloat16),
                pltpu.VMEM((experts, width), jnp.bfloat16),
                pltpu.VMEM((experts, tokens), f32),
                pltpu.VMEM((top_k, tokens), f32),
                pltpu.VMEM((experts, 128), f32),
                pltpu.VMEM((experts, 128), f32),
                pltpu.VMEM((n, 8, 256), f32),
                pltpu.VMEM((n, 8, 128), f32),
                pltpu.VMEM((slabs, experts, SLAB), f32),
                pltpu.VMEM((slabs, half, SLAB), f32),
                pltpu.VMEM((21, half, SLAB), f32),
                pltpu.SemaphoreType.DMA((tokens // TB,)),
                pltpu.SemaphoreType.DMA,
                pltpu.SemaphoreType.DMA((n,)), pltpu.SemaphoreType.DMA((n,)),
                pltpu.SemaphoreType.DMA((n,)), pltpu.SemaphoreType.DMA((n,)),
                pltpu.SemaphoreType.DMA((24,)), pltpu.SemaphoreType.DMA((24,)),
                pltpu.SemaphoreType.DMA((21,)), pltpu.SemaphoreType.DMA((21,)),
                pltpu.SemaphoreType.DMA((21,)), pltpu.SemaphoreType.DMA((21,)),
                pltpu.SemaphoreType.DMA((24,)), pltpu.SemaphoreType.DMA((24,)),
            ],
            compiler_params=pltpu.CompilerParams(collective_id=0, has_side_effects=True,
                                                 vmem_limit_bytes=40 * 2 ** 20),
        )(hidden, wt, expert_idx.T, gate_grad.T)
        rows = 256
        hg, gates, aux, rg = pl.pallas_call(
            second_kernel,
            grid=(tokens // rows,),
            out_shape=(jax.ShapeDtypeStruct((tokens, width), jnp.bfloat16),
                       jax.ShapeDtypeStruct((top_k, tokens), f32),
                       jax.ShapeDtypeStruct((1, 128), f32),
                       jax.ShapeDtypeStruct((experts, width), f32)),
            in_specs=[VMEM, VMEM, ANY, ANY, ANY],
            out_specs=(pl.BlockSpec((rows, width), lambda i: (i, 0)), ANY, ANY, ANY),
            scratch_shapes=[pltpu.VMEM((8, 128), jnp.bfloat16), pltpu.SemaphoreType.DMA((slabs + 2,))],
            compiler_params=pltpu.CompilerParams(vmem_limit_bytes=40 * 2 ** 20),
        )(gt, wt, gates, aux, rg)
        return gates.T, aux[0, 0], hg, rg.T

    return jax.shard_map(device_step, mesh=mesh,
                         in_specs=(P("dp", None), P(None, None), P("dp", None), P("dp", None)),
                         out_specs=(P("dp", None), P(), P("dp", None), P(None, None)), check_vma=False)
```

```python
import functools

import jax
import jax.numpy as jnp
from jax import lax
from jax.experimental import pallas as pl
from jax.experimental.pallas import tpu as pltpu
from jax.sharding import PartitionSpec as P

LOSS_ALPHA = 0.001
MESH = pl.DeviceIdType.MESH
TB = 256
LANES = 128
SLAB = 256
LAG = 2
FLIGHT = 4
READY = 5
HBM = pl.BlockSpec(memory_space=pltpu.HBM)
VMEM = pl.BlockSpec(memory_space=pltpu.VMEM)


def loop(lo, hi, fn):
    def step(i, carry):
        fn(i)
        return carry

    lax.fori_loop(lo, hi, step, 0)


def first_kernel(total_rows, num_devices, hid_hbm, wt_hbm, idx_hbm, gg_hbm,
                 gt_ref, gates_ref, aux_ref, out_ref, wt,
                 idx_ref, gg_ref, hid, wn, probs, pgrad, psum, flane, cnts, auxs, part, dbuf, rx,
                 isem, hsem, wsem, csem, asem, dsend, drecv, xsend, xrecv, gsend, grecv, esem):
    tokens, width = hid.shape
    experts = wt.shape[0]
    half = experts // 2
    nblk = tokens // TB
    loss_scale = float(total_rows * experts * experts)
    aux_coef = loss_scale * LOSS_ALPHA * experts / total_rows

    me = lax.axis_index("dp")
    core, bx, by, bz = me % 2, (me // 2) % 2, (me // 4) % 2, me // 8
    partner = me + 1 - 2 * core
    across = {"x": me + 2 - 4 * bx, "y": me + 4 - 8 * by, "z": me + 8 - 16 * bz}
    bits = {"x": bx, "y": by, "z": bz}
    routes = (("x", "y", "z"), ("y", "z", "x"), ("z", "x", "y"))
    mine = pl.ds(pl.multiple_of(core * half, 8), half)
    theirs = pl.ds(pl.multiple_of((1 - core) * half, 8), half)

    def hid_copy(b):
        rows = pl.ds(pl.multiple_of(b * TB, TB), TB)
        return pltpu.make_async_copy(hid_hbm.at[rows], hid.at[rows], hsem.at[b])

    def remote(src, dst, send, recv, to):
        return pltpu.make_async_remote_copy(src, dst, send, recv, device_id=(to,), device_id_type=MESH)

    idx_copy = pltpu.make_async_copy(idx_hbm, idx_ref, isem.at[0])
    gg_copy = pltpu.make_async_copy(gg_hbm, gg_ref, isem.at[1])
    w_copy = pltpu.make_async_copy(wt_hbm, wt, wsem)
    idx_copy.start()
    w_copy.start()
    gg_copy.start()
    for b in range(FLIGHT):
        hid_copy(b).start()

    barrier = pltpu.get_barrier_semaphore()
    loop(1, num_devices, lambda d: pl.semaphore_signal(
        barrier, inc=1, device_id=((me + d) % num_devices,), device_id_type=MESH))

    erows = cnts.shape[2]
    eids = lax.broadcasted_iota(jnp.int32, (experts, LANES), 0)

    def count(i, acc):
        ids = idx_ref[:, pl.ds(pl.multiple_of(i * LANES, LANES), LANES)]
        for j in range(ids.shape[0]):
            acc = acc + jnp.where(eids == ids[j:j + 1, :], 1.0, 0.0)
        return acc

    idx_copy.wait()
    local = lax.fori_loop(0, tokens // LANES, count, jnp.zeros((experts, LANES), jnp.float32))
    local = jnp.concatenate([local, jnp.zeros((erows - experts, LANES), jnp.float32)], axis=0)
    row = jnp.sum(local.T, axis=0, keepdims=True)
    cnts[0] = jnp.broadcast_to(row, (8, erows))
    psum[...] = jnp.zeros_like(psum)
    probs[:, pl.ds(tokens - TB, TB)] = jnp.zeros((experts, TB), jnp.float32)
    pl.semaphore_wait(barrier, num_devices - 1)

    def spread(buf, sem):
        loop(1, num_devices, lambda d: remote(
            buf.at[0], buf.at[d], sem.at[0], sem.at[1], (me + d) % num_devices).start())

    def gather_sum(buf, sem):
        rest = buf.at[pl.ds(1, num_devices - 1)]
        remote(rest, rest, sem.at[0], sem.at[1], partner).wait()
        tot = buf[0]
        for d in range(1, num_devices):
            tot = tot + buf[d]
        return tot

    spread(cnts, csem)
    gg_copy.wait()
    w_copy.wait()

    def turn(i):
        c = pl.ds(pl.multiple_of(i * SLAB, SLAB), SLAB)
        wn[c, :] = wt[:, c].T

    loop(0, width // SLAB, turn)

    def logits(b):
        rows = pl.ds(pl.multiple_of(b * TB, TB), TB)
        lg = jnp.dot(hid[rows, :], wn[...], preferred_element_type=jnp.float32)
        probs[:, rows] = lg.T

    groups = range(0, experts, 8)
    base = lax.broadcasted_iota(jnp.int32, (8, LANES), 0)

    def spread_rows(x):
        return [jnp.broadcast_to(x[j:j + 1, :], (8, LANES)) for j in range(x.shape[0])]

    def lanes(i):
        return pl.ds(pl.multiple_of(i * LANES, LANES), LANES)

    def forward_chunk(i):
        c = lanes(i)
        ids = [i - base for i in spread_rows(idx_ref[:, c])]
        top = probs[0:8, c]
        for g in groups[1:]:
            top = jnp.maximum(top, probs[g:g + 8, c])
        top = jnp.max(top, axis=0, keepdims=True)
        total = jnp.zeros((8, LANES), jnp.float32)
        hits = [jnp.zeros((8, LANES), jnp.float32) for _ in ids]
        for g in groups:
            ex = jnp.exp(probs[g:g + 8, c] - top)
            probs[g:g + 8, c] = ex
            total = total + ex
            for j, i in enumerate(ids):
                hits[j] = jnp.where(i == g, ex, hits[j])
        scale = 1.0 / jnp.sum(total, axis=0, keepdims=True)
        picked = jnp.concatenate([jnp.sum(h, axis=0, keepdims=True) for h in hits], axis=0) * scale
        pick_sum = jnp.sum(picked, axis=0, keepdims=True)
        gates = picked / pick_sum
        gates_ref[:, c] = gates
        sg = loss_scale * gg_ref[:, c]
        pgrad[:, c] = (sg - jnp.sum(sg * gates, axis=0, keepdims=True)) / pick_sum
        for g in groups:
            probs[g:g + 8, c] = probs[g:g + 8, c] * scale

    def backward_chunk(i):
        c = lanes(i)
        ids = [i - base for i in spread_rows(idx_ref[:, c])]
        pg = spread_rows(pgrad[:, c])
        inner = jnp.zeros((8, LANES), jnp.float32)
        grads = []
        for g in groups:
            q = jnp.zeros((8, LANES), jnp.float32)
            for j, i in enumerate(ids):
                q = jnp.where(i == g, pg[j], q)
            q = q + aux_coef * flane[g:g + 8, :]
            grads.append(q)
            p = probs[g:g + 8, c]
            psum[g:g + 8, :] += p
            inner = inner + p * q
        inner = jnp.sum(inner, axis=0, keepdims=True)
        for n in range(0, len(grads), 2):
            g = groups[n]
            lo = probs[g:g + 8, c] * (grads[n] - inner)
            hi = probs[g + 8:g + 16, c] * (grads[n + 1] - inner)
            gt_ref[g:g + 16, c] = jnp.concatenate([lo, hi], axis=0).astype(jnp.bfloat16)

    per = TB // LANES

    def arrive(b):
        hid_copy(b).wait()

        @pl.when(b + FLIGHT < nblk)
        def _():
            hid_copy(b + FLIGHT).start()

    def early(b):
        arrive(b)
        logits(b)
        last = (b + nblk - 1) % nblk
        for i in range(per):
            forward_chunk(last * per + i)

    def late(b):
        arrive(b)
        logits(b)
        for i in range(per):
            forward_chunk((b - 1) * per + i)
        for i in range(2 * per):
            backward_chunk((b - READY) * 2 * per + i)

    loop(0, READY, early)
    freq = gather_sum(cnts, csem)[0:1, :] / total_rows
    flane[...] = jnp.broadcast_to(freq, (LANES, erows)).T[:experts, :]
    loop(READY, nblk, late)
    loop((nblk - 1) * per, nblk * per, forward_chunk)
    loop((nblk - READY) * 2 * per, nblk * per, backward_chunk)

    def slab(p, k):
        far = 7 - k
        flips = (far // 4, (far // 2) % 2, far % 2)
        v = {name: bits[name] + fl - 2 * bits[name] * fl for name, fl in zip(routes[p], flips)}
        return p * 8 + v["z"] * 4 + v["y"] * 2 + v["x"]

    def dcopy(p, k):
        return remote(part.at[slab(p, k), theirs], dbuf.at[p * 8 + k], dsend, drecv.at[p * 8 + k], partner)

    def xcopy(p, k, dim):
        return remote(part.at[slab(p, k), mine], rx.at[p * 7 + k], xsend, xrecv.at[p * 7 + k],
                      across[routes[p][dim]])

    def gcopy(p, k, dim):
        s = slab(p, k)
        return remote(out_ref.at[s, mine], out_ref.at[s, mine], gsend, grecv.at[p * 7 + k - (4, 2, 1)[dim]],
                      across[routes[p][dim]])

    def ecopy(p, k):
        s = slab(p, k)
        return remote(out_ref.at[s, mine], out_ref.at[s, mine], esem.at[0], esem.at[1], partner)

    def compute(k):
        for p in range(3):
            s = slab(p, k)
            part[s] = jnp.dot(gt_ref[...], hid[:, pl.ds(pl.multiple_of(s * SLAB, SLAB), SLAB)],
                              preferred_element_type=jnp.float32)
        for p in range(3):
            dcopy(p, k).start()

    def pair_sum(k):
        for p in range(3):
            dcopy(p, k).wait_recv()
            s = slab(p, k)
            part[s, mine] = part[s, mine] + dbuf[p * 8 + k]

    def pair_send(k):
        pair_sum(k)
        for p in range(3):
            xcopy(p, k, 0).start()

    def compute_and_send(k):
        compute(k)
        pair_send(k - LAG)

    loop(0, LAG, compute)
    loop(LAG, 4 + LAG, compute_and_send)
    loop(4 + LAG, 8, compute)
    auxs[0] = jnp.broadcast_to(jnp.sum(psum[...] * flane[...]), (8, 128))
    spread(auxs, asem)
    loop(4, 8, pair_sum)

    def second(k):
        for p in range(3):
            xcopy(p, k - 4, 0).wait_recv()
            s = slab(p, k)
            part[s, mine] = part[s, mine] + rx[p * 7 + k - 4]
            xcopy(p, k, 1).start()

    loop(4, 6, second)
    for p in range(3):
        xcopy(p, 2, 0).wait_recv()
        xcopy(p, 4, 1).wait_recv()
        s = slab(p, 6)
        part[s, mine] = part[s, mine] + rx[p * 7 + 2] + rx[p * 7 + 4]
        xcopy(p, 6, 2).start()
    for p in range(3):
        xcopy(p, 3, 0).wait_recv()
        xcopy(p, 5, 1).wait_recv()
        xcopy(p, 6, 2).wait_recv()
        s = slab(p, 7)
        out_ref[s, mine] = part[s, mine] + rx[p * 7 + 3] + rx[p * 7 + 5] + rx[p * 7 + 6]
        for dim in (2, 1, 0):
            gcopy(p, 7, dim).start()
        ecopy(p, 7).start()
    for p in range(3):
        gcopy(p, 7, 2).wait_recv()
        gcopy(p, 6, 1).start()
        gcopy(p, 6, 0).start()
        ecopy(p, 6).start()

    def relay(i):
        k = 5 - i
        for p in range(3):
            gcopy(p, k + 2, 1).wait_recv()
            gcopy(p, k, 0).start()
            ecopy(p, k).start()

    def close(i):
        k = 3 - i
        for p in range(3):
            gcopy(p, k + 4, 0).wait_recv()
            ecopy(p, k).start()

    loop(0, 2, relay)
    loop(0, 4, close)
    aux_ref[...] = gather_sum(auxs, asem) * (LOSS_ALPHA * experts / total_rows)
    remote(dbuf, dbuf, dsend, drecv.at[0], partner).wait_send()
    remote(rx, rx, xsend, xrecv.at[0], partner).wait_send()
    remote(rx, rx, gsend, grecv.at[0], partner).wait_send()
    remote(dbuf, dbuf, esem.at[0], esem.at[1], partner).wait()


def second_kernel(blocks, gt_ref, wt_ref, gates_in, aux_in, rg_in, hg_ref, gates_out, aux_out, rg_out,
                  buf, sems, rsem, bsems):
    slabs = rg_in.shape[0]
    small = [pltpu.make_async_copy(gates_in, gates_out, sems.at[0]),
             pltpu.make_async_copy(aux_in.at[pl.ds(0, 1)], aux_out, sems.at[1])]
    for c in small:
        c.start()
    loop(0, slabs, lambda s: pltpu.make_async_copy(
        rg_in.at[s], rg_out.at[:, pl.ds(pl.multiple_of(s * SLAB, SLAB), SLAB)], rsem).start())
    start, sem = 0, 0
    for rows, times in blocks:
        def block(i, rows=rows, start=start, sem=sem):
            r = pl.ds(pl.multiple_of(start + i * rows, rows), rows)
            buf[r, :] = jnp.dot(gt_ref[:, r].T, wt_ref[...], preferred_element_type=jnp.float32).astype(jnp.bfloat16)
            pltpu.make_async_copy(buf.at[r], hg_ref.at[r], bsems.at[sem + i]).start()

        loop(0, times, block)
        start, sem = start + rows * times, sem + times
    for c in small:
        c.wait()
    pltpu.make_async_copy(rg_in, rg_in, rsem).wait()
    start, sem = 0, 0
    for rows, times in blocks:
        def wait(i, rows=rows, start=start, sem=sem):
            r = pl.ds(pl.multiple_of(start + i * rows, rows), rows)
            pltpu.make_async_copy(buf.at[r], hg_ref.at[r], bsems.at[sem + i]).wait()

        loop(0, times, wait)
        start, sem = start + rows * times, sem + times


def solution(mesh):
    n = mesh.shape["dp"]

    def device_step(hidden, router_w, expert_idx, gate_grad):
        tokens, width = hidden.shape
        experts = router_w.shape[1]
        top_k = expert_idx.shape[1]
        slabs = width // SLAB
        half = experts // 2
        f32 = jnp.float32
        dma = pltpu.SemaphoreType.DMA
        gt, gates, aux, rg, wt = pl.pallas_call(
            functools.partial(first_kernel, tokens * n, n),
            out_shape=(jax.ShapeDtypeStruct((experts, tokens), jnp.bfloat16),
                       jax.ShapeDtypeStruct((top_k, tokens), f32),
                       jax.ShapeDtypeStruct((8, 128), f32),
                       jax.ShapeDtypeStruct((slabs, experts, SLAB), f32),
                       jax.ShapeDtypeStruct((experts, width), jnp.bfloat16)),
            in_specs=[HBM] * 4,
            out_specs=(VMEM,) * 5,
            scratch_shapes=[
                pltpu.VMEM((top_k, tokens), jnp.int32),
                pltpu.VMEM((top_k, tokens), f32),
                pltpu.VMEM((tokens, width), jnp.bfloat16),
                pltpu.VMEM((width, experts), jnp.bfloat16),
                pltpu.VMEM((experts, tokens), f32),
                pltpu.VMEM((top_k, tokens), f32),
                pltpu.VMEM((experts, 128), f32),
                pltpu.VMEM((experts, 128), f32),
                pltpu.VMEM((n, 8, 256), f32),
                pltpu.VMEM((n, 8, 128), f32),
                pltpu.VMEM((slabs, experts, SLAB), f32),
                pltpu.VMEM((slabs, half, SLAB), f32),
                pltpu.VMEM((21, half, SLAB), f32),
                dma((2,)), dma((tokens // TB,)), dma,
                dma((2,)), dma((2,)),
                dma, dma((24,)), dma, dma((21,)), dma, dma((21,)), dma((2,)),
            ],
            compiler_params=pltpu.CompilerParams(collective_id=0, has_side_effects=True,
                                                 vmem_limit_bytes=40 * 2 ** 20),
        )(hidden, *(pltpu.with_memory_space_constraint(a, pltpu.HBM)
                    for a in (router_w.T, expert_idx.T, gate_grad.T)))
        blocks = [(256, tokens // 256 - 1), (128, 2)]
        hg, gates, aux, rg = pl.pallas_call(
            functools.partial(second_kernel, blocks),
            out_shape=(jax.ShapeDtypeStruct((tokens, width), jnp.bfloat16),
                       jax.ShapeDtypeStruct((top_k, tokens), f32),
                       jax.ShapeDtypeStruct((1, 128), f32),
                       jax.ShapeDtypeStruct((experts, width), f32)),
            in_specs=[VMEM] * 5,
            out_specs=(HBM,) * 4,
            scratch_shapes=[pltpu.VMEM((tokens, width), jnp.bfloat16), dma((2,)), dma,
                            dma((sum(t for _, t in blocks),))],
            compiler_params=pltpu.CompilerParams(vmem_limit_bytes=40 * 2 ** 20),
        )(gt, wt, gates, aux, rg)
        return gates.T, aux[0, 0], hg, rg.T

    return jax.shard_map(device_step, mesh=mesh,
                         in_specs=(P("dp", None), P(None, None), P("dp", None), P("dp", None)),
                         out_specs=(P("dp", None), P(), P("dp", None), P(None, None)), check_vma=False)
```

```python
import functools

import jax
import jax.numpy as jnp
from jax import lax
from jax.experimental import pallas as pl
from jax.experimental.pallas import tpu as pltpu
from jax.sharding import PartitionSpec as P

LOSS_ALPHA = 0.001
MESH = pl.DeviceIdType.MESH
TB = 512
COPY = 256
LANES = 128
SLAB = 256
LAG = 2
FLIGHT = 3
HBM = pl.BlockSpec(memory_space=pltpu.HBM)
VMEM = pl.BlockSpec(memory_space=pltpu.VMEM)


def loop(lo, hi, fn):
    def step(i, carry):
        fn(i)
        return carry

    lax.fori_loop(lo, hi, step, 0)


def first_kernel(total_rows, num_devices, hid_hbm, wt_hbm, idx_hbm, gg_hbm,
                 gt_ref, gates_ref, aux_ref, out_ref, wt,
                 idx_ref, gg_ref, hid, probs, pgrad, psum, flane, cnts, auxs, part, dbuf, rx,
                 isem, hsem, wsem, csem, asem, dsend, drecv, xsend, xrecv, gsend, grecv, esem):
    tokens, width = hid.shape
    experts = wt.shape[0]
    half = experts // 2
    nblk = tokens // TB
    loss_scale = float(total_rows * experts * experts)
    aux_coef = loss_scale * LOSS_ALPHA * experts / total_rows

    me = lax.axis_index("dp")
    core, bx, by, bz = me % 2, (me // 2) % 2, (me // 4) % 2, me // 8
    partner = me + 1 - 2 * core
    across = {"x": me + 2 - 4 * bx, "y": me + 4 - 8 * by, "z": me + 8 - 16 * bz}
    bits = {"x": bx, "y": by, "z": bz}
    routes = (("x", "y", "z"), ("y", "z", "x"), ("z", "x", "y"))
    mine = pl.ds(pl.multiple_of(core * half, 8), half)
    theirs = pl.ds(pl.multiple_of((1 - core) * half, 8), half)

    def hid_copy(b):
        rows = pl.ds(pl.multiple_of(b * COPY, COPY), COPY)
        return pltpu.make_async_copy(hid_hbm.at[rows], hid.at[rows], hsem.at[b])

    def remote(src, dst, send, recv, to):
        return pltpu.make_async_remote_copy(src, dst, send, recv, device_id=(to,), device_id_type=MESH)

    idx_copy = pltpu.make_async_copy(idx_hbm, idx_ref, isem.at[0])
    gg_copy = pltpu.make_async_copy(gg_hbm, gg_ref, isem.at[1])
    w_copy = pltpu.make_async_copy(wt_hbm, wt, wsem)
    idx_copy.start()
    w_copy.start()
    gg_copy.start()
    for b in range(FLIGHT):
        hid_copy(b).start()

    barrier = pltpu.get_barrier_semaphore()
    loop(1, num_devices, lambda d: pl.semaphore_signal(
        barrier, inc=1, device_id=((me + d) % num_devices,), device_id_type=MESH))

    erows = cnts.shape[2]
    groups = range(0, experts, 8)
    base = lax.broadcasted_iota(jnp.int32, (8, LANES), 0)

    def spread_rows(x):
        return [jnp.broadcast_to(x[j:j + 1, :], (8, LANES)) for j in range(x.shape[0])]

    def lanes(i):
        return pl.ds(pl.multiple_of(i * LANES, LANES), LANES)

    def count(i, acc):
        ids = [i - base for i in spread_rows(idx_ref[:, lanes(i)])]
        out = []
        for a, g in zip(acc, groups):
            for j in ids:
                a = jnp.where(j == g, a + 1.0, a)
            out.append(a)
        return tuple(out)

    idx_copy.wait()
    zero = jnp.zeros((8, LANES), jnp.float32)
    local = lax.fori_loop(0, tokens // LANES, count, (zero,) * len(groups))
    local = jnp.concatenate(list(local) + [zero] * ((erows - experts) // 8), axis=0)
    row = jnp.sum(local.T, axis=0, keepdims=True)
    cnts[0] = jnp.broadcast_to(row, (8, erows))
    psum[...] = jnp.zeros_like(psum)
    probs[:, pl.ds(tokens - TB, TB)] = jnp.zeros((experts, TB), jnp.float32)
    pl.semaphore_wait(barrier, num_devices - 1)

    def spread(buf, sem):
        loop(1, num_devices, lambda d: remote(
            buf.at[0, pl.ds(0, 1)], buf.at[d, pl.ds(0, 1)], sem.at[0], sem.at[1], (me + d) % num_devices).start())

    def gather_sum(buf, sem):
        rest = buf.at[pl.ds(1, num_devices - 1), pl.ds(0, 1)]
        remote(rest, rest, sem.at[0], sem.at[1], partner).wait()
        tot = buf[0, 0:1]
        for d in range(1, num_devices):
            tot = tot + buf[d, 0:1]
        return tot

    spread(cnts, csem)
    gg_copy.wait()
    w_copy.wait()

    def logits(b):
        rows = pl.ds(pl.multiple_of(b * TB, TB), TB)
        lg = lax.dot_general(hid[rows, :], wt[...], (((1,), (1,)), ((), ())), preferred_element_type=jnp.float32)
        probs[:, rows] = lg.T

    def forward_chunk(i):
        c = lanes(i)
        ids = [i - base for i in spread_rows(idx_ref[:, c])]
        top = probs[0:8, c]
        for g in groups[1:]:
            top = jnp.maximum(top, probs[g:g + 8, c])
        top = jnp.max(top, axis=0, keepdims=True)
        total = jnp.zeros((8, LANES), jnp.float32)
        hits = [jnp.zeros((8, LANES), jnp.float32) for _ in ids]
        for g in groups:
            ex = jnp.exp(probs[g:g + 8, c] - top)
            probs[g:g + 8, c] = ex
            total = total + ex
            for j, i in enumerate(ids):
                hits[j] = jnp.where(i == g, ex, hits[j])
        scale = 1.0 / jnp.sum(total, axis=0, keepdims=True)
        picked = jnp.concatenate([jnp.sum(h, axis=0, keepdims=True) for h in hits], axis=0) * scale
        pick_sum = jnp.sum(picked, axis=0, keepdims=True)
        gates = picked / pick_sum
        gates_ref[:, c] = gates
        sg = loss_scale * gg_ref[:, c]
        pgrad[:, c] = (sg - jnp.sum(sg * gates, axis=0, keepdims=True)) / pick_sum
        for g in groups:
            probs[g:g + 8, c] = probs[g:g + 8, c] * scale

    def backward_chunk(i):
        c = lanes(i)
        ids = [i - base for i in spread_rows(idx_ref[:, c])]
        pg = spread_rows(pgrad[:, c])
        inner = jnp.zeros((8, LANES), jnp.float32)
        grads = []
        for g in groups:
            q = jnp.zeros((8, LANES), jnp.float32)
            for j, i in enumerate(ids):
                q = jnp.where(i == g, pg[j], q)
            q = q + flane[g:g + 8, :]
            grads.append(q)
            p = probs[g:g + 8, c]
            psum[g:g + 8, :] += p
            inner = inner + p * q
        inner = jnp.sum(inner, axis=0, keepdims=True)
        for n in range(0, len(grads), 2):
            g = groups[n]
            lo = probs[g:g + 8, c] * (grads[n] - inner)
            hi = probs[g + 8:g + 16, c] * (grads[n + 1] - inner)
            gt_ref[g:g + 16, c] = jnp.concatenate([lo, hi], axis=0).astype(jnp.bfloat16)

    per = TB // LANES

    ncopy = tokens // COPY

    def arrive(b):
        for i in range(TB // COPY):
            hid_copy(b * (TB // COPY) + i).wait()
        for i in range(TB // COPY):
            nxt = b * (TB // COPY) + i + FLIGHT

            @pl.when(nxt < ncopy)
            def _():
                hid_copy(nxt).start()

    def block(b):
        arrive(b)
        logits(b)
        last = (b + nblk - 1) % nblk
        for i in range(per):
            forward_chunk(last * per + i)

    loop(0, nblk, block)
    loop((nblk - 1) * per, nblk * per, forward_chunk)
    freq = gather_sum(cnts, csem) * (aux_coef / total_rows)
    flane[...] = jnp.broadcast_to(freq, (LANES, erows)).T[:experts, :]
    loop(0, nblk * per, backward_chunk)

    def slab(p, k):
        far = 7 - k
        flips = (far // 4, (far // 2) % 2, far % 2)
        v = {name: bits[name] + fl - 2 * bits[name] * fl for name, fl in zip(routes[p], flips)}
        return p * 8 + v["z"] * 4 + v["y"] * 2 + v["x"]

    def dcopy(p, k):
        return remote(part.at[slab(p, k), theirs], dbuf.at[p * 8 + k], dsend, drecv.at[p * 8 + k], partner)

    def xcopy(p, k, dim):
        return remote(part.at[slab(p, k), mine], rx.at[p * 7 + k], xsend, xrecv.at[p * 7 + k],
                      across[routes[p][dim]])

    def gcopy(p, k, dim):
        s = slab(p, k)
        return remote(out_ref.at[s, mine], out_ref.at[s, mine], gsend, grecv.at[p * 7 + k - (4, 2, 1)[dim]],
                      across[routes[p][dim]])

    def ecopy(p, k):
        s = slab(p, k)
        return remote(out_ref.at[s, mine], out_ref.at[s, mine], esem.at[0], esem.at[1], partner)

    def compute(k):
        for p in range(3):
            s = slab(p, k)
            part[s] = jnp.dot(gt_ref[...], hid[:, pl.ds(pl.multiple_of(s * SLAB, SLAB), SLAB)],
                              preferred_element_type=jnp.float32)
        for p in range(3):
            dcopy(p, k).start()

    def pair_sum(k):
        for p in range(3):
            dcopy(p, k).wait_recv()
            s = slab(p, k)
            part[s, mine] = part[s, mine] + dbuf[p * 8 + k]

        @pl.when(k < 4)
        def _():
            for p in range(3):
                xcopy(p, k, 0).start()

    def compute_and_send(k):
        @pl.when(k >= LAG)
        def _():
            pair_sum(k - LAG)

        @pl.when(k < 8)
        def _():
            compute(k)

    loop(0, 8 + LAG, compute_and_send)
    auxs[0] = jnp.broadcast_to(jnp.sum(psum[...] * flane[...]), (8, 128))
    spread(auxs, asem)

    def second(k):
        for p in range(3):
            xcopy(p, k - 4, 0).wait_recv()
            s = slab(p, k)
            part[s, mine] = part[s, mine] + rx[p * 7 + k - 4]
            xcopy(p, k, 1).start()

    loop(4, 6, second)
    for p in range(3):
        xcopy(p, 2, 0).wait_recv()
        xcopy(p, 4, 1).wait_recv()
        s = slab(p, 6)
        part[s, mine] = part[s, mine] + rx[p * 7 + 2] + rx[p * 7 + 4]
        xcopy(p, 6, 2).start()
    for p in range(3):
        xcopy(p, 3, 0).wait_recv()
        xcopy(p, 5, 1).wait_recv()
        xcopy(p, 6, 2).wait_recv()
        s = slab(p, 7)
        out_ref[s, mine] = part[s, mine] + rx[p * 7 + 3] + rx[p * 7 + 5] + rx[p * 7 + 6]
        gcopy(p, 7, 2).start()
    for dim in (1, 0):
        for p in range(3):
            gcopy(p, 7, dim).start()
    for p in range(3):
        ecopy(p, 7).start()
    for p in range(3):
        gcopy(p, 7, 2).wait_recv()
        gcopy(p, 6, 1).start()
        gcopy(p, 6, 0).start()
        ecopy(p, 6).start()

    def relay(i):
        k = 5 - i
        for p in range(3):
            gcopy(p, k + 2, 1).wait_recv()
            gcopy(p, k, 0).start()
            ecopy(p, k).start()

    def close(i):
        k = 3 - i
        for p in range(3):
            gcopy(p, k + 4, 0).wait_recv()
            ecopy(p, k).start()

    loop(0, 2, relay)
    loop(0, 4, close)
    aux_ref[...] = jnp.broadcast_to(gather_sum(auxs, asem) / loss_scale, aux_ref.shape)
    remote(dbuf, dbuf, dsend, drecv.at[0], partner).wait_send()
    remote(rx, rx, xsend, xrecv.at[0], partner).wait_send()
    remote(rx, rx, gsend, grecv.at[0], partner).wait_send()
    remote(dbuf, dbuf, esem.at[0], esem.at[1], partner).wait()


def second_kernel(blocks, gt_ref, wt_ref, gates_in, aux_in, rg_in, hg_ref, gates_out, aux_out, rg_out,
                  buf, sems, rsem, bsems):
    slabs = rg_in.shape[0]
    small = [pltpu.make_async_copy(gates_in, gates_out, sems.at[0]),
             pltpu.make_async_copy(aux_in.at[pl.ds(0, 1)], aux_out, sems.at[1])]
    for c in small:
        c.start()
    loop(0, slabs, lambda s: pltpu.make_async_copy(
        rg_in.at[s], rg_out.at[:, pl.ds(pl.multiple_of(s * SLAB, SLAB), SLAB)], rsem).start())
    start, sem = 0, 0
    for rows, times in blocks:
        def block(i, rows=rows, start=start, sem=sem):
            r = pl.ds(pl.multiple_of(start + i * rows, rows), rows)
            buf[r, :] = jnp.dot(gt_ref[:, r].T, wt_ref[...], preferred_element_type=jnp.float32).astype(jnp.bfloat16)
            pltpu.make_async_copy(buf.at[r], hg_ref.at[r], bsems.at[sem + i]).start()

        loop(0, times, block)
        start, sem = start + rows * times, sem + times
    for c in small:
        c.wait()
    pltpu.make_async_copy(rg_in, rg_in, rsem).wait()
    start, sem = 0, 0
    for rows, times in blocks:
        def wait(i, rows=rows, start=start, sem=sem):
            r = pl.ds(pl.multiple_of(start + i * rows, rows), rows)
            pltpu.make_async_copy(buf.at[r], hg_ref.at[r], bsems.at[sem + i]).wait()

        loop(0, times, wait)
        start, sem = start + rows * times, sem + times


def solution(mesh):
    n = mesh.shape["dp"]

    def device_step(hidden, router_w, expert_idx, gate_grad):
        tokens, width = hidden.shape
        experts = router_w.shape[1]
        top_k = expert_idx.shape[1]
        slabs = width // SLAB
        half = experts // 2
        f32 = jnp.float32
        dma = pltpu.SemaphoreType.DMA
        gt, gates, aux, rg, wt = pl.pallas_call(
            functools.partial(first_kernel, tokens * n, n),
            out_shape=(jax.ShapeDtypeStruct((experts, tokens), jnp.bfloat16),
                       jax.ShapeDtypeStruct((top_k, tokens), f32),
                       jax.ShapeDtypeStruct((8, 128), f32),
                       jax.ShapeDtypeStruct((slabs, experts, SLAB), f32),
                       jax.ShapeDtypeStruct((experts, width), jnp.bfloat16)),
            in_specs=[HBM] * 4,
            out_specs=(VMEM,) * 5,
            scratch_shapes=[
                pltpu.VMEM((top_k, tokens), jnp.int32),
                pltpu.VMEM((top_k, tokens), f32),
                pltpu.VMEM((tokens, width), jnp.bfloat16),
                pltpu.VMEM((experts, tokens), f32),
                pltpu.VMEM((top_k, tokens), f32),
                pltpu.VMEM((experts, 128), f32),
                pltpu.VMEM((experts, 128), f32),
                pltpu.VMEM((n, 8, 256), f32),
                pltpu.VMEM((n, 8, 128), f32),
                pltpu.VMEM((slabs, experts, SLAB), f32),
                pltpu.VMEM((slabs, half, SLAB), f32),
                pltpu.VMEM((21, half, SLAB), f32),
                dma((2,)), dma((tokens // COPY,)), dma,
                dma((2,)), dma((2,)),
                dma, dma((24,)), dma, dma((21,)), dma, dma((21,)), dma((2,)),
            ],
            compiler_params=pltpu.CompilerParams(collective_id=0, has_side_effects=True,
                                                 vmem_limit_bytes=40 * 2 ** 20),
        )(hidden, *(pltpu.with_memory_space_constraint(a, pltpu.HBM)
                    for a in (router_w.T, expert_idx.T, gate_grad.T)))
        blocks = [(256, tokens // 256 - 1), (128, 2)]
        hg, gates, aux, rg = pl.pallas_call(
            functools.partial(second_kernel, blocks),
            out_shape=(jax.ShapeDtypeStruct((tokens, width), jnp.bfloat16),
                       jax.ShapeDtypeStruct((top_k, tokens), f32),
                       jax.ShapeDtypeStruct((1, 128), f32),
                       jax.ShapeDtypeStruct((experts, width), f32)),
            in_specs=[VMEM] * 5,
            out_specs=(HBM,) * 4,
            scratch_shapes=[pltpu.VMEM((tokens, width), jnp.bfloat16), dma((2,)), dma,
                            dma((sum(t for _, t in blocks),))],
            compiler_params=pltpu.CompilerParams(vmem_limit_bytes=40 * 2 ** 20),
        )(gt, wt, gates, aux, rg)
        return gates.T, aux[0, 0], hg, rg.T

    return jax.shard_map(device_step, mesh=mesh,
                         in_specs=(P("dp", None), P(None, None), P("dp", None), P("dp", None)),
                         out_specs=(P("dp", None), P(), P("dp", None), P(None, None)), check_vma=False)
```

```python
import functools

import jax
import jax.numpy as jnp
from jax import lax
from jax.experimental import pallas as pl
from jax.experimental.pallas import tpu as pltpu
from jax.sharding import PartitionSpec as P

LOSS_ALPHA = 0.001
MESH = pl.DeviceIdType.MESH
TB = 512
COPY = 256
LANES = 128
SLAB = 256
LAG = 2
ROWS = 256
EARLY = 2
FLIGHT = 3
HBM = pl.BlockSpec(memory_space=pltpu.HBM)
VMEM = pl.BlockSpec(memory_space=pltpu.VMEM)


def loop(lo, hi, fn):
    def step(i, carry):
        fn(i)
        return carry

    lax.fori_loop(lo, hi, step, 0)


def first_kernel(total_rows, num_devices, hid_hbm, wt_hbm, idx_hbm, gg_hbm,
                 gt_ref, gates_ref, aux_ref, out_ref, wt, hg_ref,
                 idx_ref, gg_ref, hid, probs, pgrad, psum, flane, cnts, auxs, part, dbuf, rx,
                 isem, hsem, wsem, csem, asem, dsend, drecv, xsend, xrecv, gsend, grecv, esem):
    tokens, width = hid.shape
    experts = wt.shape[0]
    half = experts // 2
    nblk = tokens // TB
    loss_scale = float(total_rows * experts * experts)
    aux_coef = loss_scale * LOSS_ALPHA * experts / total_rows

    me = lax.axis_index("dp")
    core, bx, by, bz = me % 2, (me // 2) % 2, (me // 4) % 2, me // 8
    partner = me + 1 - 2 * core
    mine = pl.ds(pl.multiple_of(core * half, 8), half)
    theirs = pl.ds(pl.multiple_of((1 - core) * half, 8), half)

    def hid_copy(b):
        rows = pl.ds(pl.multiple_of(b * COPY, COPY), COPY)
        return pltpu.make_async_copy(hid_hbm.at[rows], hid.at[rows], hsem.at[b])

    def remote(src, dst, send, recv, to):
        return pltpu.make_async_remote_copy(src, dst, send, recv, device_id=(to,), device_id_type=MESH)

    idx_copy = pltpu.make_async_copy(idx_hbm, idx_ref, isem.at[0])
    gg_copy = pltpu.make_async_copy(gg_hbm, gg_ref, isem.at[1])
    w_copy = pltpu.make_async_copy(wt_hbm, wt, wsem)
    idx_copy.start()
    w_copy.start()
    gg_copy.start()
    for b in range(FLIGHT):
        hid_copy(b).start()

    barrier = pltpu.get_barrier_semaphore()
    loop(1, num_devices, lambda d: pl.semaphore_signal(
        barrier, inc=1, device_id=((me + d) % num_devices,), device_id_type=MESH))

    erows = cnts.shape[2]
    groups = range(0, experts, 8)
    base = lax.broadcasted_iota(jnp.int32, (8, LANES), 0)

    def spread_rows(x):
        return [jnp.broadcast_to(x[j:j + 1, :], (8, LANES)) for j in range(x.shape[0])]

    def lanes(i):
        return pl.ds(pl.multiple_of(i * LANES, LANES), LANES)

    def count(i, acc):
        ids = [i - base for i in spread_rows(idx_ref[:, lanes(i)])]
        out = []
        for a, g in zip(acc, groups):
            for j in ids:
                a = jnp.where(j == g, a + 1.0, a)
            out.append(a)
        return tuple(out)

    idx_copy.wait()
    zero = jnp.zeros((8, LANES), jnp.float32)
    local = lax.fori_loop(0, tokens // LANES, count, (zero,) * len(groups))
    local = jnp.concatenate(list(local) + [zero] * ((erows - experts) // 8), axis=0)
    row = jnp.sum(local.T, axis=0, keepdims=True)
    cnts[0] = jnp.broadcast_to(row, (8, erows))
    psum[...] = jnp.zeros_like(psum)
    probs[:, pl.ds(tokens - TB, TB)] = jnp.zeros((experts, TB), jnp.float32)
    pl.semaphore_wait(barrier, num_devices - 1)

    def spread(buf, sem):
        loop(1, num_devices, lambda d: remote(
            buf.at[0, pl.ds(0, 1)], buf.at[d, pl.ds(0, 1)], sem.at[0], sem.at[1], (me + d) % num_devices).start())

    def gather_sum(buf, sem):
        rest = buf.at[pl.ds(1, num_devices - 1), pl.ds(0, 1)]
        remote(rest, rest, sem.at[0], sem.at[1], partner).wait()
        tot = buf[0, 0:1]
        for d in range(1, num_devices):
            tot = tot + buf[d, 0:1]
        return tot

    spread(cnts, csem)
    gg_copy.wait()
    w_copy.wait()

    def logits(b):
        rows = pl.ds(pl.multiple_of(b * TB, TB), TB)
        lg = lax.dot_general(hid[rows, :], wt[...], (((1,), (1,)), ((), ())), preferred_element_type=jnp.float32)
        probs[:, rows] = lg.T

    def forward_chunk(i):
        c = lanes(i)
        ids = [i - base for i in spread_rows(idx_ref[:, c])]
        top = probs[0:8, c]
        for g in groups[1:]:
            top = jnp.maximum(top, probs[g:g + 8, c])
        top = jnp.max(top, axis=0, keepdims=True)
        total = jnp.zeros((8, LANES), jnp.float32)
        hits = [jnp.zeros((8, LANES), jnp.float32) for _ in ids]
        for g in groups:
            ex = jnp.exp(probs[g:g + 8, c] - top)
            probs[g:g + 8, c] = ex
            total = total + ex
            for j, i in enumerate(ids):
                hits[j] = jnp.where(i == g, ex, hits[j])
        scale = 1.0 / jnp.sum(total, axis=0, keepdims=True)
        picked = jnp.concatenate([jnp.sum(h, axis=0, keepdims=True) for h in hits], axis=0) * scale
        pick_sum = jnp.sum(picked, axis=0, keepdims=True)
        gates = picked / pick_sum
        gates_ref[:, c] = gates
        sg = loss_scale * gg_ref[:, c]
        pgrad[:, c] = (sg - jnp.sum(sg * gates, axis=0, keepdims=True)) / pick_sum
        for g in groups:
            probs[g:g + 8, c] = probs[g:g + 8, c] * scale

    def backward_chunk(i):
        c = lanes(i)
        ids = [i - base for i in spread_rows(idx_ref[:, c])]
        pg = spread_rows(pgrad[:, c])
        inner = jnp.zeros((8, LANES), jnp.float32)
        grads = []
        for g in groups:
            q = jnp.zeros((8, LANES), jnp.float32)
            for j, i in enumerate(ids):
                q = jnp.where(i == g, pg[j], q)
            q = q + flane[g:g + 8, :]
            grads.append(q)
            p = probs[g:g + 8, c]
            psum[g:g + 8, :] += p
            inner = inner + p * q
        inner = jnp.sum(inner, axis=0, keepdims=True)
        for n in range(0, len(grads), 2):
            g = groups[n]
            lo = probs[g:g + 8, c] * (grads[n] - inner)
            hi = probs[g + 8:g + 16, c] * (grads[n + 1] - inner)
            gt_ref[g:g + 16, c] = jnp.concatenate([lo, hi], axis=0).astype(jnp.bfloat16)

    per = TB // LANES

    ncopy = tokens // COPY

    def arrive(b):
        for i in range(TB // COPY):
            hid_copy(b * (TB // COPY) + i).wait()
        for i in range(TB // COPY):
            nxt = b * (TB // COPY) + i + FLIGHT

            @pl.when(nxt < ncopy)
            def _():
                hid_copy(nxt).start()

    def block(b):
        arrive(b)
        logits(b)
        last = (b + nblk - 1) % nblk
        for i in range(per):
            forward_chunk(last * per + i)

    loop(0, nblk, block)
    loop((nblk - 1) * per, nblk * per, forward_chunk)
    freq = gather_sum(cnts, csem) * (aux_coef / total_rows)
    flane[...] = jnp.broadcast_to(freq, (LANES, erows)).T[:experts, :]
    loop(0, nblk * per, backward_chunk)

    axis_bits = (bx, by, bz)

    def slab(p, k):
        far = 7 - k
        s = p * 8
        for a in range(3):
            i = (a + 3 - p) % 3
            flip = (far // ((8 - 5 * i + i * i) // 2)) % 2
            s = s + (1, 2, 4)[a] * (axis_bits[a] + flip - 2 * axis_bits[a] * flip)
        return s

    def across(p, dim):
        a = (p + dim) % 3
        stride = 2 + a + a * a
        return me + stride * (1 - 2 * ((me // stride) % 2))

    def dcopy(p, k):
        return remote(part.at[slab(p, k), theirs], dbuf.at[p * 8 + k], dsend, drecv.at[p * 8 + k], partner)

    def xcopy(p, k, dim):
        return remote(part.at[slab(p, k), mine], rx.at[p * 7 + k], xsend, xrecv.at[p * 7 + k],
                      across(p, dim))

    def gcopy(p, k, dim):
        s = slab(p, k)
        return remote(out_ref.at[s, mine], out_ref.at[s, mine], gsend, grecv.at[p * 7 + k - (4, 2, 1)[dim]],
                      across(p, dim))

    def ecopy(p, k):
        s = slab(p, k)
        return remote(out_ref.at[s, mine], out_ref.at[s, mine], esem.at[0], esem.at[1], partner)

    def compute(k):
        for p in range(3):
            s = slab(p, k)
            part[s] = jnp.dot(gt_ref[...], hid[:, pl.ds(pl.multiple_of(s * SLAB, SLAB), SLAB)],
                              preferred_element_type=jnp.float32)
        for p in range(3):
            dcopy(p, k).start()

    def pair_sum(k):
        for p in range(3):
            dcopy(p, k).wait_recv()
            s = slab(p, k)
            part[s, mine] = part[s, mine] + dbuf[p * 8 + k]

        @pl.when(k < 4)
        def _():
            for p in range(3):
                xcopy(p, k, 0).start()

    def second(k):
        def one(p):
            xcopy(p, k - 4, 0).wait_recv()
            s = slab(p, k)
            part[s, mine] = part[s, mine] + rx[p * 7 + k - 4]
            xcopy(p, k, 1).start()

        loop(0, 3, one)

    def order(i):
        return i + ((i + 3) // 4) % 2 * (2 * (i % 2) - 1)

    def compute_and_send(i):
        @pl.when(i == LAG + 4)
        def _():
            second(4)

        @pl.when(i >= LAG)
        def _():
            pair_sum(order(i - LAG))

        @pl.when(i < 8)
        def _():
            compute(order(i))

    loop(0, 8 + LAG, compute_and_send)
    second(5)

    def hidden_rows(i):
        r = pl.ds(pl.multiple_of(i * ROWS, ROWS), ROWS)
        hg_ref[r, :] = jnp.dot(gt_ref[:, r].T, wt[...], preferred_element_type=jnp.float32).astype(jnp.bfloat16)

    def third(p):
        xcopy(p, 2, 0).wait_recv()
        xcopy(p, 4, 1).wait_recv()
        s = slab(p, 6)
        part[s, mine] = part[s, mine] + rx[p * 7 + 2] + rx[p * 7 + 4]
        xcopy(p, 6, 2).start()

    loop(0, 3, third)
    loop(0, EARLY, hidden_rows)
    auxs[0] = jnp.broadcast_to(jnp.sum(psum[...] * flane[...]), (8, 128))
    spread(auxs, asem)

    def final(p):
        xcopy(p, 3, 0).wait_recv()
        xcopy(p, 5, 1).wait_recv()
        xcopy(p, 6, 2).wait_recv()
        s = slab(p, 7)
        out_ref[s, mine] = part[s, mine] + rx[p * 7 + 3] + rx[p * 7 + 5] + rx[p * 7 + 6]
        gcopy(p, 7, 2).start()

    loop(0, 3, final)

    def own(dim):
        def one(p):
            gcopy(p, 7, dim).start()

        loop(0, 3, one)

    def pair(k):
        def one(p):
            ecopy(p, k).start()

        loop(0, 3, one)

    own(1)
    own(0)
    pair(7)

    def relay_second(p):
        gcopy(p, 7, 2).wait_recv()
        gcopy(p, 6, 1).start()

    def relay_first(p):
        gcopy(p, 6, 0).start()
        ecopy(p, 6).start()

    loop(0, 3, relay_second)
    loop(0, 3, relay_first)

    def relay(i):
        k, p = 5 - i // 3, i % 3
        gcopy(p, k + 2, 1).wait_recv()
        gcopy(p, k, 0).start()
        ecopy(p, k).start()

    def close(i):
        k, p = 3 - i // 3, i % 3
        gcopy(p, k + 4, 0).wait_recv()
        ecopy(p, k).start()

    loop(0, 6, relay)
    loop(0, 12, close)
    aux_ref[...] = jnp.broadcast_to(gather_sum(auxs, asem) / loss_scale, aux_ref.shape)
    remote(dbuf, dbuf, dsend, drecv.at[0], partner).wait_send()
    remote(rx, rx, xsend, xrecv.at[0], partner).wait_send()
    remote(rx, rx, gsend, grecv.at[0], partner).wait_send()
    remote(dbuf, dbuf, esem.at[0], esem.at[1], partner).wait()


def second_kernel(blocks, gt_ref, wt_ref, hg_in, gates_in, aux_in, rg_in, hg_ref, gates_out, aux_out, rg_out,
                  buf, sems, rsem, bsems):
    slabs = rg_in.shape[0]
    early = hg_in.shape[0]
    small = [pltpu.make_async_copy(hg_in, hg_ref.at[pl.ds(0, early)], sems.at[2]),
             pltpu.make_async_copy(gates_in, gates_out, sems.at[0]),
             pltpu.make_async_copy(aux_in.at[pl.ds(0, 1)], aux_out, sems.at[1])]
    for c in small:
        c.start()
    loop(0, slabs, lambda s: pltpu.make_async_copy(
        rg_in.at[s], rg_out.at[:, pl.ds(pl.multiple_of(s * SLAB, SLAB), SLAB)], rsem).start())
    start, sem = early, 0
    for rows, times in blocks:
        def block(i, rows=rows, start=start, sem=sem):
            r = pl.ds(pl.multiple_of(start + i * rows, rows), rows)
            here = pl.ds(pl.multiple_of(start - early + i * rows, rows), rows)
            buf[here, :] = jnp.dot(gt_ref[:, r].T, wt_ref[...], preferred_element_type=jnp.float32).astype(jnp.bfloat16)
            pltpu.make_async_copy(buf.at[here], hg_ref.at[r], bsems.at[sem + i]).start()

        loop(0, times, block)
        start, sem = start + rows * times, sem + times
    for c in small:
        c.wait()
    pltpu.make_async_copy(rg_in, rg_in, rsem).wait()
    start, sem = early, 0
    for rows, times in blocks:
        def wait(i, rows=rows, start=start, sem=sem):
            r = pl.ds(pl.multiple_of(start + i * rows, rows), rows)
            pltpu.make_async_copy(buf.at[pl.ds(0, rows)], hg_ref.at[r], bsems.at[sem + i]).wait()

        loop(0, times, wait)
        start, sem = start + rows * times, sem + times


def solution(mesh):
    n = mesh.shape["dp"]

    def device_step(hidden, router_w, expert_idx, gate_grad):
        tokens, width = hidden.shape
        experts = router_w.shape[1]
        top_k = expert_idx.shape[1]
        slabs = width // SLAB
        half = experts // 2
        f32 = jnp.float32
        dma = pltpu.SemaphoreType.DMA
        gt, gates, aux, rg, wt, head = pl.pallas_call(
            functools.partial(first_kernel, tokens * n, n),
            out_shape=(jax.ShapeDtypeStruct((experts, tokens), jnp.bfloat16),
                       jax.ShapeDtypeStruct((top_k, tokens), f32),
                       jax.ShapeDtypeStruct((8, 128), f32),
                       jax.ShapeDtypeStruct((slabs, experts, SLAB), f32),
                       jax.ShapeDtypeStruct((experts, width), jnp.bfloat16),
                       jax.ShapeDtypeStruct((EARLY * ROWS, width), jnp.bfloat16)),
            in_specs=[HBM] * 4,
            out_specs=(VMEM,) * 6,
            scratch_shapes=[
                pltpu.VMEM((top_k, tokens), jnp.int32),
                pltpu.VMEM((top_k, tokens), f32),
                pltpu.VMEM((tokens, width), jnp.bfloat16),
                pltpu.VMEM((experts, tokens), f32),
                pltpu.VMEM((top_k, tokens), f32),
                pltpu.VMEM((experts, 128), f32),
                pltpu.VMEM((experts, 128), f32),
                pltpu.VMEM((n, 8, 256), f32),
                pltpu.VMEM((n, 8, 128), f32),
                pltpu.VMEM((slabs, experts, SLAB), f32),
                pltpu.VMEM((slabs, half, SLAB), f32),
                pltpu.VMEM((21, half, SLAB), f32),
                dma((2,)), dma((tokens // COPY,)), dma,
                dma((2,)), dma((2,)),
                dma, dma((24,)), dma, dma((21,)), dma, dma((21,)), dma((2,)),
            ],
            compiler_params=pltpu.CompilerParams(collective_id=0, has_side_effects=True,
                                                 vmem_limit_bytes=40 * 2 ** 20),
        )(hidden, *(pltpu.with_memory_space_constraint(a, pltpu.HBM)
                    for a in (router_w.T, expert_idx.T, gate_grad.T)))
        rest = tokens - EARLY * ROWS
        blocks = [(ROWS, rest // ROWS)]
        hg, gates, aux, rg = pl.pallas_call(
            functools.partial(second_kernel, blocks),
            out_shape=(jax.ShapeDtypeStruct((tokens, width), jnp.bfloat16),
                       jax.ShapeDtypeStruct((top_k, tokens), f32),
                       jax.ShapeDtypeStruct((1, 128), f32),
                       jax.ShapeDtypeStruct((experts, width), f32)),
            in_specs=[VMEM] * 6,
            out_specs=(HBM,) * 4,
            scratch_shapes=[pltpu.VMEM((rest, width), jnp.bfloat16), dma((3,)), dma,
                            dma((sum(t for _, t in blocks),))],
            compiler_params=pltpu.CompilerParams(vmem_limit_bytes=40 * 2 ** 20),
        )(gt, wt, head, gates, aux, rg)
        return gates.T, aux[0, 0], hg, rg.T

    return jax.shard_map(device_step, mesh=mesh,
                         in_specs=(P("dp", None), P(None, None), P("dp", None), P("dp", None)),
                         out_specs=(P("dp", None), P(), P("dp", None), P(None, None)), check_vma=False)
```

```python
import functools

import jax
import jax.numpy as jnp
from jax import lax
from jax.experimental import pallas as pl
from jax.experimental.pallas import tpu as pltpu
from jax.sharding import PartitionSpec as P

LOSS_ALPHA = 0.001
MESH = pl.DeviceIdType.MESH
TB = 512
COPY = 256
LANES = 128
SLAB = 256
LAG = 2
ROWS = 256
EARLY = 2
FLIGHT = 3
HBM = pl.BlockSpec(memory_space=pltpu.HBM)
VMEM = pl.BlockSpec(memory_space=pltpu.VMEM)


def loop(lo, hi, fn):
    def step(i, carry):
        fn(i)
        return carry

    lax.fori_loop(lo, hi, step, 0)


def first_kernel(total_rows, num_devices, hid_hbm, wt_hbm, idx_hbm, gg_hbm,
                 gt_ref, gates_ref, aux_ref, out_ref, wt, hg_ref,
                 idx_ref, gg_ref, hid, probs, pgrad, psum, flane, cnts, auxs, part, dbuf, rx,
                 isem, hsem, wsem, csem, asem, dsend, drecv, xsend, xrecv, gsend, esem):
    tokens, width = hid.shape
    experts = wt.shape[0]
    half = experts // 2
    nblk = tokens // TB
    loss_scale = float(total_rows * experts * experts)
    aux_coef = loss_scale * LOSS_ALPHA * experts / total_rows

    me = lax.axis_index("dp")
    core, bx, by, bz = me % 2, (me // 2) % 2, (me // 4) % 2, me // 8
    partner = me + 1 - 2 * core
    mine = pl.ds(pl.multiple_of(core * half, 8), half)
    theirs = pl.ds(pl.multiple_of((1 - core) * half, 8), half)

    def hid_copy(b):
        rows = pl.ds(pl.multiple_of(b * COPY, COPY), COPY)
        return pltpu.make_async_copy(hid_hbm.at[rows], hid.at[rows], hsem.at[b])

    def remote(src, dst, send, recv, to):
        return pltpu.make_async_remote_copy(src, dst, send, recv, device_id=(to,), device_id_type=MESH)

    idx_copy = pltpu.make_async_copy(idx_hbm, idx_ref, isem.at[0])
    gg_copy = pltpu.make_async_copy(gg_hbm, gg_ref, isem.at[1])
    w_copy = pltpu.make_async_copy(wt_hbm, wt, wsem)
    idx_copy.start()
    w_copy.start()
    gg_copy.start()
    for b in range(FLIGHT):
        hid_copy(b).start()

    barrier = pltpu.get_barrier_semaphore()
    loop(1, num_devices, lambda d: pl.semaphore_signal(
        barrier, inc=1, device_id=((me + d) % num_devices,), device_id_type=MESH))

    erows = cnts.shape[2]
    groups = range(0, experts, 8)
    base = lax.broadcasted_iota(jnp.int32, (8, LANES), 0)

    def spread_rows(x):
        return [jnp.broadcast_to(x[j:j + 1, :], (8, LANES)) for j in range(x.shape[0])]

    def lanes(i):
        return pl.ds(pl.multiple_of(i * LANES, LANES), LANES)

    def count(i, acc):
        ids = [i - base for i in spread_rows(idx_ref[:, lanes(i)])]
        out = []
        for a, g in zip(acc, groups):
            for j in ids:
                a = jnp.where(j == g, a + 1.0, a)
            out.append(a)
        return tuple(out)

    idx_copy.wait()
    zero = jnp.zeros((8, LANES), jnp.float32)
    local = lax.fori_loop(0, tokens // LANES, count, (zero,) * len(groups))
    local = jnp.concatenate(list(local) + [zero] * ((erows - experts) // 8), axis=0)
    row = jnp.sum(local.T, axis=0, keepdims=True)
    cnts[0] = jnp.broadcast_to(row, (8, erows))
    psum[...] = jnp.zeros_like(psum)
    probs[:, pl.ds(tokens - TB, TB)] = jnp.zeros((experts, TB), jnp.float32)
    pl.semaphore_wait(barrier, num_devices - 1)

    def spread(buf, sem):
        loop(1, num_devices, lambda d: remote(
            buf.at[0, pl.ds(0, 1)], buf.at[d, pl.ds(0, 1)], sem.at[0], sem.at[1], (me + d) % num_devices).start())

    def gather_sum(buf, sem):
        rest = buf.at[pl.ds(1, num_devices - 1), pl.ds(0, 1)]
        remote(rest, rest, sem.at[0], sem.at[1], partner).wait()
        tot = buf[0, 0:1]
        for d in range(1, num_devices):
            tot = tot + buf[d, 0:1]
        return tot

    spread(cnts, csem)
    gg_copy.wait()
    w_copy.wait()

    def logits(b):
        rows = pl.ds(pl.multiple_of(b * TB, TB), TB)
        lg = lax.dot_general(hid[rows, :], wt[...], (((1,), (1,)), ((), ())), preferred_element_type=jnp.float32)
        probs[:, rows] = lg.T

    def forward_chunk(i):
        c = lanes(i)
        ids = [i - base for i in spread_rows(idx_ref[:, c])]
        top = probs[0:8, c]
        for g in groups[1:]:
            top = jnp.maximum(top, probs[g:g + 8, c])
        top = jnp.max(top, axis=0, keepdims=True)
        total = jnp.zeros((8, LANES), jnp.float32)
        hits = [jnp.zeros((8, LANES), jnp.float32) for _ in ids]
        for g in groups:
            ex = jnp.exp(probs[g:g + 8, c] - top)
            probs[g:g + 8, c] = ex
            total = total + ex
            for j, i in enumerate(ids):
                hits[j] = jnp.where(i == g, ex, hits[j])
        scale = 1.0 / jnp.sum(total, axis=0, keepdims=True)
        picked = jnp.concatenate([jnp.sum(h, axis=0, keepdims=True) for h in hits], axis=0) * scale
        pick_sum = jnp.sum(picked, axis=0, keepdims=True)
        gates = picked / pick_sum
        gates_ref[:, c] = gates
        sg = loss_scale * gg_ref[:, c]
        pgrad[:, c] = (sg - jnp.sum(sg * gates, axis=0, keepdims=True)) / pick_sum
        for g in groups:
            probs[g:g + 8, c] = probs[g:g + 8, c] * scale

    def backward_chunk(i):
        c = lanes(i)
        ids = [i - base for i in spread_rows(idx_ref[:, c])]
        pg = spread_rows(pgrad[:, c])
        inner = jnp.zeros((8, LANES), jnp.float32)
        grads = []
        for g in groups:
            q = jnp.zeros((8, LANES), jnp.float32)
            for j, i in enumerate(ids):
                q = jnp.where(i == g, pg[j], q)
            q = q + flane[g:g + 8, :]
            grads.append(q)
            p = probs[g:g + 8, c]
            psum[g:g + 8, :] += p
            inner = inner + p * q
        inner = jnp.sum(inner, axis=0, keepdims=True)
        for n in range(0, len(grads), 2):
            g = groups[n]
            lo = probs[g:g + 8, c] * (grads[n] - inner)
            hi = probs[g + 8:g + 16, c] * (grads[n + 1] - inner)
            gt_ref[g:g + 16, c] = jnp.concatenate([lo, hi], axis=0).astype(jnp.bfloat16)

    per = TB // LANES

    ncopy = tokens // COPY

    def arrive(b):
        for i in range(TB // COPY):
            hid_copy(b * (TB // COPY) + i).wait()
        for i in range(TB // COPY):
            nxt = b * (TB // COPY) + i + FLIGHT

            @pl.when(nxt < ncopy)
            def _():
                hid_copy(nxt).start()

    def block(b):
        arrive(b)
        logits(b)
        last = (b + nblk - 1) % nblk
        for i in range(per):
            forward_chunk(last * per + i)

    loop(0, nblk, block)
    def forward_pair(i):
        forward_chunk(2 * i)
        forward_chunk(2 * i + 1)

    loop((nblk - 1) * per // 2, nblk * per // 2, forward_pair)
    freq = gather_sum(cnts, csem) * (aux_coef / total_rows)
    flane[...] = jnp.broadcast_to(freq, (LANES, erows)).T[:experts, :]
    def backward_pair(i):
        backward_chunk(2 * i)
        backward_chunk(2 * i + 1)

    loop(0, nblk * per // 2, backward_pair)

    axis_bits = (bx, by, bz)

    def slab(p, k):
        far = 7 - k
        s = p * 8
        for a in range(3):
            i = (a + 3 - p) % 3
            flip = (far // ((8 - 5 * i + i * i) // 2)) % 2
            s = s + (1, 2, 4)[a] * (axis_bits[a] + flip - 2 * axis_bits[a] * flip)
        return s

    def across(p, dim):
        a = (p + dim) % 3
        stride = 2 + a + a * a
        return me + stride * (1 - 2 * ((me // stride) % 2))

    def dcopy(p, k):
        return remote(part.at[slab(p, k), theirs], dbuf.at[p * 8 + k], dsend, drecv.at[k], partner)

    def xcopy(p, k, dim):
        group = k if dim == 0 else 3 if k > 4 else 2
        return remote(part.at[slab(p, k), mine], rx.at[p * 7 + k], xsend, xrecv.at[group], across(p, dim))

    def arrived(sem, units):
        ref = rx.at[pl.ds(0, 3 * units)]
        remote(ref, ref, xsend, sem, partner).wait_recv()

    def gcopy(p, k, dim):
        s = slab(p, k)
        return remote(out_ref.at[s, mine], out_ref.at[s, mine], gsend, drecv.at[k - (4, 2, 1)[dim]],
                      across(p, dim))

    def ecopy(p, k):
        s = slab(p, k)
        return remote(out_ref.at[s, mine], out_ref.at[s, mine], esem.at[0], esem.at[1], partner)

    def compute(k):
        for p in range(3):
            s = slab(p, k)
            part[s] = jnp.dot(gt_ref[...], hid[:, pl.ds(pl.multiple_of(s * SLAB, SLAB), SLAB)],
                              preferred_element_type=jnp.float32)
        for p in range(3):
            dcopy(p, k).start()

    def pair_sum(k):
        arrived(drecv.at[k], 1)
        for p in range(3):
            s = slab(p, k)
            part[s, mine] = part[s, mine] + dbuf[p * 8 + k]

        @pl.when(k < 4)
        def _():
            for p in range(3):
                xcopy(p, k, 0).start()

    def second(k):
        arrived(xrecv.at[k - 4], 1)

        def one(p):
            s = slab(p, k)
            part[s, mine] = part[s, mine] + rx[p * 7 + k - 4]
            xcopy(p, k, 1).start()

        loop(0, 3, one)

    def order(i):
        return i + ((i + 3) // 4) % 2 * (2 * (i % 2) - 1)

    def compute_and_send(i):
        @pl.when(i == LAG + 4)
        def _():
            second(4)

        @pl.when(i >= LAG)
        def _():
            pair_sum(order(i - LAG))

        @pl.when(i < 8)
        def _():
            compute(order(i))

    loop(0, 8 + LAG, compute_and_send)
    second(5)

    def hidden_rows(i):
        r = pl.ds(pl.multiple_of(i * ROWS, ROWS), ROWS)
        hg_ref[r, :] = jnp.dot(gt_ref[:, r].T, wt[...], preferred_element_type=jnp.float32).astype(jnp.bfloat16)

    arrived(xrecv.at[2], 2)

    def third(p):
        s = slab(p, 6)
        part[s, mine] = part[s, mine] + rx[p * 7 + 2] + rx[p * 7 + 4]
        xcopy(p, 6, 2).start()

    loop(0, 3, third)
    loop(0, EARLY, hidden_rows)
    auxs[0] = jnp.broadcast_to(jnp.sum(psum[...] * flane[...]), (8, 128))
    spread(auxs, asem)

    arrived(xrecv.at[3], 3)

    def final(p):
        s = slab(p, 7)
        out_ref[s, mine] = part[s, mine] + rx[p * 7 + 3] + rx[p * 7 + 5] + rx[p * 7 + 6]
        gcopy(p, 7, 2).start()

    loop(0, 3, final)

    def pair(k):
        def one(p):
            ecopy(p, k).start()

        loop(0, 3, one)


    def forward_on(k, dim):
        def one(p):
            gcopy(p, k, dim).start()

        loop(0, 3, one)

    forward_on(7, 1)
    forward_on(7, 0)
    pair(7)
    arrived(drecv.at[6], 1)
    forward_on(6, 1)
    forward_on(6, 0)
    pair(6)

    def relay(i):
        arrived(drecv.at[5 - i], 1)
        forward_on(5 - i, 0)
        pair(5 - i)

    def close(i):
        arrived(drecv.at[3 - i], 1)
        pair(3 - i)

    loop(0, 2, relay)
    loop(0, 4, close)
    aux_ref[...] = jnp.broadcast_to(gather_sum(auxs, asem) / loss_scale, aux_ref.shape)
    remote(dbuf, dbuf, dsend, drecv.at[0], partner).wait_send()
    remote(rx, rx, xsend, xrecv.at[0], partner).wait_send()
    remote(rx, rx, gsend, drecv.at[0], partner).wait_send()
    remote(dbuf, dbuf, esem.at[0], esem.at[1], partner).wait()


def second_kernel(blocks, gt_ref, wt_ref, hg_in, gates_in, aux_in, rg_in, hg_ref, gates_out, aux_out, rg_out,
                  buf, sems, rsem, bsems):
    slabs = rg_in.shape[0]
    early = hg_in.shape[0]
    small = [pltpu.make_async_copy(hg_in, hg_ref.at[pl.ds(0, early)], sems.at[2]),
             pltpu.make_async_copy(gates_in, gates_out, sems.at[0]),
             pltpu.make_async_copy(aux_in.at[pl.ds(0, 1)], aux_out, sems.at[1])]
    for c in small:
        c.start()
    loop(0, slabs, lambda s: pltpu.make_async_copy(
        rg_in.at[s], rg_out.at[:, pl.ds(pl.multiple_of(s * SLAB, SLAB), SLAB)], rsem).start())
    start, sem = early, 0
    for rows, times in blocks:
        def block(i, rows=rows, start=start, sem=sem):
            r = pl.ds(pl.multiple_of(start + i * rows, rows), rows)
            here = pl.ds(pl.multiple_of(start - early + i * rows, rows), rows)
            buf[here, :] = jnp.dot(gt_ref[:, r].T, wt_ref[...], preferred_element_type=jnp.float32).astype(jnp.bfloat16)
            pltpu.make_async_copy(buf.at[here], hg_ref.at[r], bsems.at[sem + i]).start()

        loop(0, times, block)
        start, sem = start + rows * times, sem + times
    for c in small:
        c.wait()
    pltpu.make_async_copy(rg_in, rg_in, rsem).wait()
    start, sem = early, 0
    for rows, times in blocks:
        def wait(i, rows=rows, start=start, sem=sem):
            r = pl.ds(pl.multiple_of(start + i * rows, rows), rows)
            pltpu.make_async_copy(buf.at[pl.ds(0, rows)], hg_ref.at[r], bsems.at[sem + i]).wait()

        loop(0, times, wait)
        start, sem = start + rows * times, sem + times


def solution(mesh):
    n = mesh.shape["dp"]

    def device_step(hidden, router_w, expert_idx, gate_grad):
        tokens, width = hidden.shape
        experts = router_w.shape[1]
        top_k = expert_idx.shape[1]
        slabs = width // SLAB
        half = experts // 2
        f32 = jnp.float32
        dma = pltpu.SemaphoreType.DMA
        gt, gates, aux, rg, wt, head = pl.pallas_call(
            functools.partial(first_kernel, tokens * n, n),
            out_shape=(jax.ShapeDtypeStruct((experts, tokens), jnp.bfloat16),
                       jax.ShapeDtypeStruct((top_k, tokens), f32),
                       jax.ShapeDtypeStruct((8, 128), f32),
                       jax.ShapeDtypeStruct((slabs, experts, SLAB), f32),
                       jax.ShapeDtypeStruct((experts, width), jnp.bfloat16),
                       jax.ShapeDtypeStruct((EARLY * ROWS, width), jnp.bfloat16)),
            in_specs=[HBM] * 4,
            out_specs=(VMEM,) * 6,
            scratch_shapes=[
                pltpu.VMEM((top_k, tokens), jnp.int32),
                pltpu.VMEM((top_k, tokens), f32),
                pltpu.VMEM((tokens, width), jnp.bfloat16),
                pltpu.VMEM((experts, tokens), f32),
                pltpu.VMEM((top_k, tokens), f32),
                pltpu.VMEM((experts, 128), f32),
                pltpu.VMEM((experts, 128), f32),
                pltpu.VMEM((n, 8, 256), f32),
                pltpu.VMEM((n, 8, 128), f32),
                pltpu.VMEM((slabs, experts, SLAB), f32),
                pltpu.VMEM((slabs, half, SLAB), f32),
                pltpu.VMEM((21, half, SLAB), f32),
                dma((2,)), dma((tokens // COPY,)), dma,
                dma((2,)), dma((2,)),
                dma, dma((8,)), dma, dma((4,)), dma, dma((2,)),
            ],
            compiler_params=pltpu.CompilerParams(collective_id=0, has_side_effects=True,
                                                 vmem_limit_bytes=40 * 2 ** 20),
        )(hidden, *(pltpu.with_memory_space_constraint(a, pltpu.HBM)
                    for a in (router_w.T, expert_idx.T, gate_grad.T)))
        rest = tokens - EARLY * ROWS
        blocks = [(ROWS, rest // ROWS)]
        hg, gates, aux, rg = pl.pallas_call(
            functools.partial(second_kernel, blocks),
            out_shape=(jax.ShapeDtypeStruct((tokens, width), jnp.bfloat16),
                       jax.ShapeDtypeStruct((top_k, tokens), f32),
                       jax.ShapeDtypeStruct((1, 128), f32),
                       jax.ShapeDtypeStruct((experts, width), f32)),
            in_specs=[VMEM] * 6,
            out_specs=(HBM,) * 4,
            scratch_shapes=[pltpu.VMEM((rest, width), jnp.bfloat16), dma((3,)), dma,
                            dma((sum(t for _, t in blocks),))],
            compiler_params=pltpu.CompilerParams(vmem_limit_bytes=40 * 2 ** 20),
        )(gt, wt, head, gates, aux, rg)
        return gates.T, aux[0, 0], hg, rg.T

    return jax.shard_map(device_step, mesh=mesh,
                         in_specs=(P("dp", None), P(None, None), P("dp", None), P("dp", None)),
                         out_specs=(P("dp", None), P(), P("dp", None), P(None, None)), check_vma=False)
```

```python
import functools

import jax
import jax.numpy as jnp
from jax import lax
from jax.experimental import pallas as pl
from jax.experimental.pallas import tpu as pltpu
from jax.sharding import PartitionSpec as P

LOSS_ALPHA = 0.001
MESH = pl.DeviceIdType.MESH
TB = 512
COPY = 256
LANES = 128
SLAB = 256
LAG = 3
ROWS = 256
EARLY = 2
FLIGHT = 3
HBM = pl.BlockSpec(memory_space=pltpu.HBM)
VMEM = pl.BlockSpec(memory_space=pltpu.VMEM)


def loop(lo, hi, fn):
    def step(i, carry):
        fn(i)
        return carry

    lax.fori_loop(lo, hi, step, 0)


def first_kernel(total_rows, num_devices, hid_hbm, wt_hbm, idx_hbm, gg_hbm,
                 gt_ref, gates_ref, aux_ref, out_ref, wt, hg_ref,
                 idx_ref, gg_ref, hid, probs, pgrad, psum, flane, cnts, auxs, part, dbuf, rx,
                 isem, hsem, wsem, csem, asem, dsend, drecv, xsend, xrecv, gsend, esem):
    tokens, width = hid.shape
    experts = wt.shape[0]
    half = experts // 2
    nblk = tokens // TB
    loss_scale = float(total_rows * experts * experts)
    aux_coef = loss_scale * LOSS_ALPHA * experts / total_rows

    me = lax.axis_index("dp")
    core, bx, by, bz = me % 2, (me // 2) % 2, (me // 4) % 2, me // 8
    partner = me + 1 - 2 * core
    mine = pl.ds(pl.multiple_of(core * half, 8), half)
    theirs = pl.ds(pl.multiple_of((1 - core) * half, 8), half)

    def hid_copy(b):
        rows = pl.ds(pl.multiple_of(b * COPY, COPY), COPY)
        return pltpu.make_async_copy(hid_hbm.at[rows], hid.at[rows], hsem.at[b])

    def remote(src, dst, send, recv, to):
        return pltpu.make_async_remote_copy(src, dst, send, recv, device_id=(to,), device_id_type=MESH)

    idx_copy = pltpu.make_async_copy(idx_hbm, idx_ref, isem.at[0])
    gg_copy = pltpu.make_async_copy(gg_hbm, gg_ref, isem.at[1])
    w_copy = pltpu.make_async_copy(wt_hbm, wt, wsem)
    idx_copy.start()
    w_copy.start()
    gg_copy.start()
    for b in range(FLIGHT):
        hid_copy(b).start()

    barrier = pltpu.get_barrier_semaphore()
    loop(1, num_devices, lambda d: pl.semaphore_signal(
        barrier, inc=1, device_id=((me + d) % num_devices,), device_id_type=MESH))

    erows = cnts.shape[2]
    groups = range(0, experts, 8)
    base = lax.broadcasted_iota(jnp.int32, (8, LANES), 0)

    def spread_rows(x):
        return [jnp.broadcast_to(x[j:j + 1, :], (8, LANES)) for j in range(x.shape[0])]

    def lanes(i):
        return pl.ds(pl.multiple_of(i * LANES, LANES), LANES)

    def count(i, acc):
        ids = [i - base for i in spread_rows(idx_ref[:, lanes(i)])]
        out = []
        for a, g in zip(acc, groups):
            for j in ids:
                a = jnp.where(j == g, a + 1.0, a)
            out.append(a)
        return tuple(out)

    idx_copy.wait()
    zero = jnp.zeros((8, LANES), jnp.float32)
    local = lax.fori_loop(0, tokens // LANES, count, (zero,) * len(groups))
    local = jnp.concatenate(list(local) + [zero] * ((erows - experts) // 8), axis=0)
    row = jnp.sum(local.T, axis=0, keepdims=True)
    cnts[0] = jnp.broadcast_to(row, (8, erows))
    psum[...] = jnp.zeros_like(psum)
    probs[:, pl.ds(tokens - TB, TB)] = jnp.zeros((experts, TB), jnp.float32)
    pl.semaphore_wait(barrier, num_devices - 1)

    def spread(buf, sem):
        loop(1, num_devices, lambda d: remote(
            buf.at[0, pl.ds(0, 1)], buf.at[d, pl.ds(0, 1)], sem.at[0], sem.at[1], (me + d) % num_devices).start())

    def gather_sum(buf, sem):
        rest = buf.at[pl.ds(1, num_devices - 1), pl.ds(0, 1)]
        remote(rest, rest, sem.at[0], sem.at[1], partner).wait()
        tot = buf[0, 0:1]
        for d in range(1, num_devices):
            tot = tot + buf[d, 0:1]
        return tot

    spread(cnts, csem)
    gg_copy.wait()
    w_copy.wait()

    def logits(b):
        rows = pl.ds(pl.multiple_of(b * TB, TB), TB)
        lg = lax.dot_general(hid[rows, :], wt[...], (((1,), (1,)), ((), ())), preferred_element_type=jnp.float32)
        probs[:, rows] = lg.T

    def forward_chunk(i):
        c = lanes(i)
        ids = [i - base for i in spread_rows(idx_ref[:, c])]
        top = probs[0:8, c]
        for g in groups[1:]:
            top = jnp.maximum(top, probs[g:g + 8, c])
        top = jnp.max(top, axis=0, keepdims=True)
        total = jnp.zeros((8, LANES), jnp.float32)
        hits = [jnp.zeros((8, LANES), jnp.float32) for _ in ids]
        for g in groups:
            ex = jnp.exp(probs[g:g + 8, c] - top)
            probs[g:g + 8, c] = ex
            total = total + ex
            for j, i in enumerate(ids):
                hits[j] = jnp.where(i == g, ex, hits[j])
        scale = 1.0 / jnp.sum(total, axis=0, keepdims=True)
        picked = jnp.concatenate([jnp.sum(h, axis=0, keepdims=True) for h in hits], axis=0) * scale
        pick_sum = jnp.sum(picked, axis=0, keepdims=True)
        gates = picked / pick_sum
        gates_ref[:, c] = gates
        sg = loss_scale * gg_ref[:, c]
        pgrad[:, c] = (sg - jnp.sum(sg * gates, axis=0, keepdims=True)) / pick_sum
        for g in groups:
            probs[g:g + 8, c] = probs[g:g + 8, c] * scale

    def backward_chunk(i):
        c = lanes(i)
        ids = [i - base for i in spread_rows(idx_ref[:, c])]
        pg = spread_rows(pgrad[:, c])
        inner = jnp.zeros((8, LANES), jnp.float32)
        grads = []
        for g in groups:
            q = jnp.zeros((8, LANES), jnp.float32)
            for j, i in enumerate(ids):
                q = jnp.where(i == g, pg[j], q)
            q = q + flane[g:g + 8, :]
            grads.append(q)
            p = probs[g:g + 8, c]
            psum[g:g + 8, :] += p
            inner = inner + p * q
        inner = jnp.sum(inner, axis=0, keepdims=True)
        for n in range(0, len(grads), 2):
            g = groups[n]
            lo = probs[g:g + 8, c] * (grads[n] - inner)
            hi = probs[g + 8:g + 16, c] * (grads[n + 1] - inner)
            gt_ref[g:g + 16, c] = jnp.concatenate([lo, hi], axis=0).astype(jnp.bfloat16)

    per = TB // LANES

    ncopy = tokens // COPY

    def arrive(b):
        for i in range(TB // COPY):
            hid_copy(b * (TB // COPY) + i).wait()
        for i in range(TB // COPY):
            nxt = b * (TB // COPY) + i + FLIGHT

            @pl.when(nxt < ncopy)
            def _():
                hid_copy(nxt).start()

    def block(b):
        arrive(b)
        logits(b)
        last = (b + nblk - 1) % nblk
        for i in range(per):
            forward_chunk(last * per + i)

    loop(0, nblk, block)
    def forward_pair(i):
        forward_chunk(2 * i)
        forward_chunk(2 * i + 1)

    loop((nblk - 1) * per // 2, nblk * per // 2, forward_pair)
    freq = gather_sum(cnts, csem) * (aux_coef / total_rows)
    flane[...] = jnp.broadcast_to(freq, (LANES, erows)).T[:experts, :]
    def backward_pair(i):
        backward_chunk(2 * i)
        backward_chunk(2 * i + 1)

    loop(0, nblk * per // 2, backward_pair)

    axis_bits = (bx, by, bz)

    def slab(p, k):
        far = 7 - k
        s = p * 8
        for a in range(3):
            i = (a + 3 - p) % 3
            flip = (far // ((8 - 5 * i + i * i) // 2)) % 2
            s = s + (1, 2, 4)[a] * (axis_bits[a] + flip - 2 * axis_bits[a] * flip)
        return s

    def across(p, dim):
        a = (p + dim) % 3
        stride = 2 + a + a * a
        return me + stride * (1 - 2 * ((me // stride) % 2))

    def dcopy(p, k):
        return remote(part.at[slab(p, k), theirs], dbuf.at[p * 8 + k], dsend, drecv.at[k], partner)

    def xcopy(p, k, dim):
        group = k if dim == 0 else 3 if k > 4 else 2
        return remote(part.at[slab(p, k), mine], rx.at[p * 7 + k], xsend, xrecv.at[group], across(p, dim))

    def arrived(sem, units):
        ref = rx.at[pl.ds(0, 3 * units)]
        remote(ref, ref, xsend, sem, partner).wait_recv()

    def gcopy(p, k, dim):
        s = slab(p, k)
        return remote(out_ref.at[s, mine], out_ref.at[s, mine], gsend, drecv.at[k - (4, 2, 1)[dim]],
                      across(p, dim))

    def ecopy(p, k):
        s = slab(p, k)
        return remote(out_ref.at[s, mine], out_ref.at[s, mine], esem.at[0], esem.at[1], partner)

    def compute(k):
        for p in range(3):
            s = slab(p, k)
            part[s] = jnp.dot(gt_ref[...], hid[:, pl.ds(pl.multiple_of(s * SLAB, SLAB), SLAB)],
                              preferred_element_type=jnp.float32)
        for p in range(3):
            dcopy(p, k).start()

    def pair_sum(k):
        arrived(drecv.at[k], 1)
        for p in range(3):
            s = slab(p, k)
            part[s, mine] = part[s, mine] + dbuf[p * 8 + k]

        @pl.when(k < 4)
        def _():
            for p in range(3):
                xcopy(p, k, 0).start()

    def second(k):
        arrived(xrecv.at[k - 4], 1)

        def one(p):
            s = slab(p, k)
            part[s, mine] = part[s, mine] + rx[p * 7 + k - 4]
            xcopy(p, k, 1).start()

        loop(0, 3, one)

    def order(i):
        return i + ((i + 3) // 4) % 2 * (2 * (i % 2) - 1)

    def compute_and_send(i):
        @pl.when(i == LAG + 4)
        def _():
            second(4)

        @pl.when(i >= LAG)
        def _():
            pair_sum(order(i - LAG))

        @pl.when(i < 8)
        def _():
            compute(order(i))

    loop(0, 8 + LAG, compute_and_send)
    second(5)

    def hidden_rows(i):
        r = pl.ds(pl.multiple_of(i * ROWS, ROWS), ROWS)
        hg_ref[r, :] = jnp.dot(gt_ref[:, r].T, wt[...], preferred_element_type=jnp.float32).astype(jnp.bfloat16)

    arrived(xrecv.at[2], 2)

    def third(p):
        s = slab(p, 6)
        part[s, mine] = part[s, mine] + rx[p * 7 + 2] + rx[p * 7 + 4]
        xcopy(p, 6, 2).start()

    loop(0, 3, third)
    loop(0, EARLY, hidden_rows)
    auxs[0] = jnp.broadcast_to(jnp.sum(psum[...] * flane[...]), (8, 128))
    spread(auxs, asem)

    arrived(xrecv.at[3], 3)

    def final(p):
        s = slab(p, 7)
        out_ref[s, mine] = part[s, mine] + rx[p * 7 + 3] + rx[p * 7 + 5] + rx[p * 7 + 6]
        gcopy(p, 7, 2).start()

    loop(0, 3, final)

    def pair(k):
        def one(p):
            ecopy(p, k).start()

        loop(0, 3, one)


    def forward_on(k, dim):
        def one(p):
            gcopy(p, k, dim).start()

        loop(0, 3, one)

    forward_on(7, 1)
    forward_on(7, 0)
    pair(7)
    arrived(drecv.at[6], 1)
    forward_on(6, 1)
    forward_on(6, 0)
    pair(6)

    def relay(i):
        arrived(drecv.at[5 - i], 1)
        forward_on(5 - i, 0)
        pair(5 - i)

    def close(i):
        arrived(drecv.at[3 - i], 1)
        pair(3 - i)

    loop(0, 2, relay)
    loop(0, 4, close)
    aux_ref[...] = jnp.broadcast_to(gather_sum(auxs, asem) / loss_scale, aux_ref.shape)
    remote(dbuf, dbuf, dsend, drecv.at[0], partner).wait_send()
    remote(rx, rx, xsend, xrecv.at[0], partner).wait_send()
    remote(rx, rx, gsend, drecv.at[0], partner).wait_send()
    remote(dbuf, dbuf, esem.at[0], esem.at[1], partner).wait()


def second_kernel(blocks, gt_ref, wt_ref, hg_in, gates_in, aux_in, rg_in, hg_ref, gates_out, aux_out, rg_out,
                  buf, sems, rsem, bsems):
    slabs = rg_in.shape[0]
    early = hg_in.shape[0]
    small = [pltpu.make_async_copy(hg_in, hg_ref.at[pl.ds(0, early)], sems.at[2]),
             pltpu.make_async_copy(gates_in, gates_out, sems.at[0]),
             pltpu.make_async_copy(aux_in.at[pl.ds(0, 1)], aux_out, sems.at[1])]
    for c in small:
        c.start()
    loop(0, slabs, lambda s: pltpu.make_async_copy(
        rg_in.at[s], rg_out.at[:, pl.ds(pl.multiple_of(s * SLAB, SLAB), SLAB)], rsem).start())
    start, sem = early, 0
    for rows, times in blocks:
        def block(i, rows=rows, start=start, sem=sem):
            r = pl.ds(pl.multiple_of(start + i * rows, rows), rows)
            here = pl.ds(pl.multiple_of(start - early + i * rows, rows), rows)
            buf[here, :] = jnp.dot(gt_ref[:, r].T, wt_ref[...], preferred_element_type=jnp.float32).astype(jnp.bfloat16)
            pltpu.make_async_copy(buf.at[here], hg_ref.at[r], bsems.at[sem + i]).start()

        loop(0, times, block)
        start, sem = start + rows * times, sem + times
    for c in small:
        c.wait()
    pltpu.make_async_copy(rg_in, rg_in, rsem).wait()
    start, sem = early, 0
    for rows, times in blocks:
        def wait(i, rows=rows, start=start, sem=sem):
            r = pl.ds(pl.multiple_of(start + i * rows, rows), rows)
            pltpu.make_async_copy(buf.at[pl.ds(0, rows)], hg_ref.at[r], bsems.at[sem + i]).wait()

        loop(0, times, wait)
        start, sem = start + rows * times, sem + times


def solution(mesh):
    n = mesh.shape["dp"]

    def device_step(hidden, router_w, expert_idx, gate_grad):
        tokens, width = hidden.shape
        experts = router_w.shape[1]
        top_k = expert_idx.shape[1]
        slabs = width // SLAB
        half = experts // 2
        f32 = jnp.float32
        dma = pltpu.SemaphoreType.DMA
        gt, gates, aux, rg, wt, head = pl.pallas_call(
            functools.partial(first_kernel, tokens * n, n),
            out_shape=(jax.ShapeDtypeStruct((experts, tokens), jnp.bfloat16),
                       jax.ShapeDtypeStruct((top_k, tokens), f32),
                       jax.ShapeDtypeStruct((8, 128), f32),
                       jax.ShapeDtypeStruct((slabs, experts, SLAB), f32),
                       jax.ShapeDtypeStruct((experts, width), jnp.bfloat16),
                       jax.ShapeDtypeStruct((EARLY * ROWS, width), jnp.bfloat16)),
            in_specs=[HBM] * 4,
            out_specs=(VMEM,) * 6,
            scratch_shapes=[
                pltpu.VMEM((top_k, tokens), jnp.int32),
                pltpu.VMEM((top_k, tokens), f32),
                pltpu.VMEM((tokens, width), jnp.bfloat16),
                pltpu.VMEM((experts, tokens), f32),
                pltpu.VMEM((top_k, tokens), f32),
                pltpu.VMEM((experts, 128), f32),
                pltpu.VMEM((experts, 128), f32),
                pltpu.VMEM((n, 8, 256), f32),
                pltpu.VMEM((n, 8, 128), f32),
                pltpu.VMEM((slabs, experts, SLAB), f32),
                pltpu.VMEM((slabs, half, SLAB), f32),
                pltpu.VMEM((21, half, SLAB), f32),
                dma((2,)), dma((tokens // COPY,)), dma,
                dma((2,)), dma((2,)),
                dma, dma((8,)), dma, dma((4,)), dma, dma((2,)),
            ],
            compiler_params=pltpu.CompilerParams(collective_id=0, has_side_effects=True,
                                                 vmem_limit_bytes=40 * 2 ** 20),
        )(hidden, *(pltpu.with_memory_space_constraint(a, pltpu.HBM)
                    for a in (router_w.T, expert_idx.T, gate_grad.T)))
        rest = tokens - EARLY * ROWS
        blocks = [(ROWS, rest // ROWS)]
        hg, gates, aux, rg = pl.pallas_call(
            functools.partial(second_kernel, blocks),
            out_shape=(jax.ShapeDtypeStruct((tokens, width), jnp.bfloat16),
                       jax.ShapeDtypeStruct((top_k, tokens), f32),
                       jax.ShapeDtypeStruct((1, 128), f32),
                       jax.ShapeDtypeStruct((experts, width), f32)),
            in_specs=[VMEM] * 6,
            out_specs=(HBM,) * 4,
            scratch_shapes=[pltpu.VMEM((rest, width), jnp.bfloat16), dma((3,)), dma,
                            dma((sum(t for _, t in blocks),))],
            compiler_params=pltpu.CompilerParams(vmem_limit_bytes=40 * 2 ** 20),
        )(gt, wt, head, gates, aux, rg)
        return gates.T, aux[0, 0], hg, rg.T

    return jax.shard_map(device_step, mesh=mesh,
                         in_specs=(P("dp", None), P(None, None), P("dp", None), P("dp", None)),
                         out_specs=(P("dp", None), P(), P("dp", None), P(None, None)), check_vma=False)
```
